128 devices in a mesh: grp: 4 (over z), dev: 32 (over x, y, core).
Axes of the slice: x: 4, y: 4, z: 4, core: 2. Of those that a mesh axis runs over, the one named last changes fastest.
Arguments:
- qkv_weight: bfloat16 [2, 4608, 8192], P(None, ('grp', 'dev')), may hold values from -0.09375 to 0.09375
- gate_up_weight: bfloat16 [2, 4608, 73728], P(None, ('grp', 'dev')), may hold values from -0.09375 to 0.09375
- head_slot: int32 [64], replicated, may hold values from 0 to 63, each once
- layer_ids: int32 [2], replicated, may hold values from 0 to 45
- stored_qkv: int32 [46, 64], replicated, may hold values from -16384 to 16383
- stored_gate_up: int32 [46, 576], replicated, may hold values from -16384 to 16383
Outputs:
- served_qkv: bfloat16 [2, 4608, 8192], P(None, 'grp', 'dev')
- served_gate_up: bfloat16 [2, 4608, 73728], P(None, 'grp', 'dev')
- qkv_mismatch: float32 [2, 64], P(None, 'dev')
- gate_up_mismatch: float32 [2, 576], P(None, 'dev')
The draws below stay inside these ranges and needn't reach their ends.
Inputs may be any that keep to these rules, and one draw needn't show every extreme that they name: `head_slot`: each of the 64 heads appears once.
All inputs are finite; a program needn't handle non-finite values.
Results may differ from the reference program's by a relative error of at most 0.0004.
Values may be sent and summed in bfloat16 or wider, within the bound.
A program may use at most 128 MiB of HBM per device.

```python
import jax
import jax.numpy as jnp
from jax import lax

D = 4608
HEAD_DIM = 128
FF = 36864
STORED = 46
LAYERS = 2
BLK = 128
NHEAD = 64
N_DEV = 32


def touch_ends(values, key, low, largest):
    place = [jax.random.randint(jax.random.fold_in(key, axis), (), 0, length) for axis, length in enumerate(values.shape)]
    longest = values.shape.index(max(values.shape))
    next_to = place[:longest] + [(place[longest] + 1) % values.shape[longest]] + place[longest + 1:]
    return values.at[tuple(place)].set(low).at[tuple(next_to)].set(largest)


def steps_of(rng, shape, split, smallest, high):
    factor_of, own = 1.0, jax.random.fold_in(rng, 6)
    for axis_at, shards_of in split:
        draws = jnp.exp(jax.random.uniform(jax.random.fold_in(own, axis_at), (shards_of,), jnp.float32, smallest / len(split), high / len(split)))
        factor_of = factor_of * jnp.repeat(draws, shape[axis_at] // shards_of).reshape([-1 if axis == axis_at else 1 for axis in range(len(shape))])
    return factor_of


def centred(key, dims, spread, bound, split=(), dtype=jnp.bfloat16):
    factor_of = steps_of(key, dims, split, -0.22, 0.18) if split else 1.0
    values = jax.random.normal(key, dims, jnp.float32) * spread * factor_of
    return jnp.minimum(jnp.maximum(values, -bound), bound).astype(dtype)


def setup_inputs(seed: int = 0) -> dict:
    key_of = jax.random.split(jax.random.key(seed), 7)
    return {
        "qkv_weight": centred(key_of[0], (LAYERS, D, NHEAD * HEAD_DIM), D ** -0.5, 0.09375, ((1, 128),)),
        "gate_up_weight": centred(key_of[1], (LAYERS, D, 2 * FF), D ** -0.5, 0.09375, ((1, 128),)),
        "head_slot": jax.random.permutation(key_of[2], NHEAD).astype(jnp.int32),
        "layer_ids": jax.random.randint(key_of[3], (LAYERS,), 0, STORED).astype(jnp.int32),
        "stored_qkv": touch_ends(jax.random.randint(key_of[4], (STORED, NHEAD), -16384, 16384), jax.random.fold_in(key_of[4], 1), -16384, 16383).astype(jnp.int32),
        "stored_gate_up": touch_ends(jax.random.randint(key_of[5], (STORED, 2 * FF // BLK), -16384, 16384), jax.random.fold_in(key_of[5], 1), -16384, 16383).astype(jnp.int32),
    }


stored_unit = 1.0 / 1024.0


def reference(qkv_weight, gate_up_weight, head_slot, layer_ids, stored_qkv, stored_gate_up):
    width = FF // N_DEV
    served_qkv = qkv_weight.reshape(LAYERS, D, NHEAD, HEAD_DIM)[:, :, head_slot, :].reshape(LAYERS, D, NHEAD * HEAD_DIM)
    served_gate_up = gate_up_weight.reshape(LAYERS, D, 2, N_DEV, width).transpose(0, 1, 3, 2, 4).reshape(LAYERS, D, 2 * FF)

    def layer_sums(pair):
        qkv_layer, gate_layer = pair
        head_sum = jnp.sum(qkv_layer.astype(jnp.float32).reshape(D, NHEAD, HEAD_DIM), axis=(0, 2))
        block_sum = jnp.sum(gate_layer.astype(jnp.float32).reshape(D, 2 * FF // BLK, BLK), axis=(0, 2))
        return head_sum, block_sum

    head_sum, block_sum = lax.map(layer_sums, (served_qkv, served_gate_up))
    picked_qkv = stored_qkv[layer_ids][:, head_slot].astype(jnp.float32)
    picked_gate = stored_gate_up[layer_ids].reshape(LAYERS, 2, N_DEV, width // BLK)
    picked_gate = picked_gate.transpose(0, 2, 1, 3).reshape(LAYERS, 2 * FF // BLK).astype(jnp.float32)
    qkv_mismatch = head_sum - picked_qkv * stored_unit
    gate_up_mismatch = block_sum - picked_gate * stored_unit
    return served_qkv, served_gate_up, qkv_mismatch, gate_up_mismatch
```

```python
import functools

import jax
import jax.numpy as jnp
from jax import lax
from jax.experimental import pallas as pl
from jax.experimental.pallas import tpu as pltpu
from jax.sharding import PartitionSpec as P

HEAD_DIM = 128
FF = 36864
STORED = 46
BLK = 128
NHEAD = 64
LAYERS = 2
ROWS = 36
N_DEV = 32
N_GRP = 4
WIDTH = FF // N_DEV
BLOCKS = WIDTH // BLK
SLOTS = NHEAD // N_DEV
QW = SLOTS * HEAD_DIM

stored_unit = 1.0 / 1024.0
MESH = pl.DeviceIdType.MESH

FAR_X = ((2, 1, 0, 1), (0, 1, 0, 1), (2, -1, 0, 1), (0, -1, 0, 1))
FAR_Y = ((1, 2, 1, 0), (-1, 0, 1, 0), (-1, 2, 1, 0), (1, 0, 1, 0))
DIAGONAL = ((1, 1, 1, 0), (-1, -1, 1, 0), (1, -1, 1, 0), (-1, 1, 1, 0))
OPPOSITE = ((2, 0, 0, 0), (0, 2, 0, 0), (2, 2, 0, 0))
ROUNDS = (FAR_X, FAR_Y, DIAGONAL, OPPOSITE)


def owner_at(me, offset, flip):
    dx, dy, mirror_x, mirror_y = offset
    x, y, core = me // 8, (me // 2) % 4, me % 2
    sign = 1 - 2 * core
    x = (x + (dx * sign if mirror_x else dx) + 4) % 4
    y = (y + (dy * sign if mirror_y else dy) + 4) % 4
    return (x * 4 + y) * 2 + (core + flip) % 2


def kernel(
    gate, qkv, slot_ref, layer_ref, stored_q, stored_g,
    gate_out, qkv_out, mismatch,
    qkv_in, qkv_send, rows_in, sum_send, sum_recv, part_send, part_recv, table_q, table_g,
    gate_sem, qkv_sem, sum_sem, part_sem, own_sem, load_sem, table_sem,
):
    me = lax.axis_index("dev")
    grp = lax.axis_index("grp")

    load_tq = pltpu.make_async_copy(stored_q, table_q, table_sem.at[1])
    load_tg = pltpu.make_async_copy(stored_g, table_g, table_sem.at[2])

    def load_head(head, _):
        column = pl.ds(pl.multiple_of(head * HEAD_DIM, HEAD_DIM), HEAD_DIM)
        pltpu.make_async_copy(qkv.at[:, :, column], qkv_in.at[head], table_sem.at[0]).start()
        return 0

    lax.fori_loop(0, NHEAD, load_head, 0)
    load_tq.start()
    load_tg.start()

    barrier = pltpu.get_barrier_semaphore()

    def greet(k, _):
        pl.semaphore_signal(barrier, inc=1, device_id={"dev": (me + k) % N_DEV}, device_id_type=MESH)
        return 0

    lax.fori_loop(1, N_DEV, greet, 0)
    for k in range(1, N_GRP):
        pl.semaphore_signal(barrier, inc=1, device_id={"grp": (grp + k) % N_GRP}, device_id_type=MESH)
    pl.semaphore_wait(barrier, N_DEV + N_GRP - 2)

    own_rows = pl.ds(me * ROWS, ROWS)

    def send_gate(owner, p):
        pltpu.make_async_remote_copy(
            src_ref=gate.at[:, :, pl.ds(pl.multiple_of(p * FF + owner * WIDTH, BLK), WIDTH)],
            dst_ref=gate_out.at[own_rows, :, pl.ds(pl.multiple_of(p * WIDTH, BLK), WIDTH)],
            send_sem=gate_sem.at[0],
            recv_sem=gate_sem.at[1],
            device_id={"dev": owner},
            device_id_type=MESH,
        ).start()

    def send_qkv(owner):
        pltpu.make_async_remote_copy(
            src_ref=qkv_send.at[owner],
            dst_ref=qkv_out.at[own_rows],
            send_sem=qkv_sem.at[0],
            recv_sem=qkv_sem.at[1],
            device_id={"dev": owner},
            device_id_type=MESH,
        ).start()

    def gate_round(offsets):
        def step(i, _):
            for offset in offsets:
                send_gate(owner_at(me, offset, i % 2), i // 2)
            return 0

        lax.fori_loop(0, 4, step, 0)

    partner = owner_at(me, (0, 0, 0, 0), 1)
    own_copies = []
    for p in range(2):
        send_gate(partner, p)
        own_copies.append(
            pltpu.make_async_copy(
                gate.at[:, :, pl.ds(pl.multiple_of(p * FF + me * WIDTH, BLK), WIDTH)],
                gate_out.at[own_rows, :, pl.ds(p * WIDTH, WIDTH)],
                own_sem.at[p],
            )
        )
    gate_round(ROUNDS[0])
    gate_round(ROUNDS[1])
    for copy in own_copies:
        copy.start()

    pltpu.make_async_copy(qkv_in, qkv_in, table_sem.at[0]).wait()

    def place(slot, _):
        part = qkv_in[slot_ref[slot]]
        column = pl.ds(pl.multiple_of((slot % SLOTS) * HEAD_DIM, HEAD_DIM), HEAD_DIM)
        qkv_send[slot // SLOTS, :, :, column] = part
        return 0

    lax.fori_loop(0, NHEAD, place, 0)

    def load(owner, slot):
        return [
            pltpu.make_async_copy(
                gate.at[:, :, pl.ds(pl.multiple_of(p * FF + owner * WIDTH, BLK), WIDTH)],
                rows_in.at[slot, p],
                load_sem.at[slot, p],
            )
            for p in range(2)
        ]

    lane = lax.broadcasted_iota(jnp.int32, (LAYERS, 128), 1)

    def block_total(values, at, total):
        rows = jnp.sum(values.astype(jnp.float32), axis=0)
        return jnp.where(lane == at, jnp.sum(rows, axis=1, keepdims=True), total)

    for copy in load(0, 0):
        copy.start()

    def add_up(owner, _):
        slot = owner % 2

        @pl.when(owner + 1 < N_DEV)
        def _():
            for copy in load(owner + 1, 1 - slot):
                copy.start()

        for copy in load(owner, slot):
            copy.wait()
        total = jnp.zeros((LAYERS, 128), jnp.float32)
        for p in range(2):
            for b in range(BLOCKS):
                total = block_total(rows_in[slot, p, :, :, b * BLK : (b + 1) * BLK], p * BLOCKS + b, total)
        for s in range(SLOTS):
            total = block_total(
                qkv_send[owner, :, :, s * HEAD_DIM : (s + 1) * HEAD_DIM], 2 * BLOCKS + s, total
            )
        sum_send[owner] = total
        return 0

    lax.fori_loop(0, N_DEV, add_up, 0)

    own_copies.append(pltpu.make_async_copy(qkv_send.at[me], qkv_out.at[own_rows], own_sem.at[2]))
    own_copies[2].start()

    def send_qkv_round(offsets, flip):
        for offset in offsets:
            send_qkv(owner_at(me, offset, flip))

    def small_sends(i, _):
        owner = (me + i) % N_DEV
        pltpu.make_async_remote_copy(
            src_ref=sum_send.at[owner],
            dst_ref=sum_recv.at[me],
            send_sem=sum_sem.at[0],
            recv_sem=sum_sem.at[1],
            device_id={"dev": owner},
            device_id_type=MESH,
        ).start()
        return 0

    lax.fori_loop(1, N_DEV, small_sends, 0)
    send_qkv(partner)

    def qkv_sends(flip, _):
        for offsets in ROUNDS:
            send_qkv_round(offsets, flip)
        return 0

    lax.fori_loop(0, 2, qkv_sends, 0)
    gate_round(ROUNDS[2])
    gate_round(ROUNDS[3])

    sum_recv[me] = sum_send[me]

    load_tq.wait()
    load_tg.wait()
    row_of = lax.broadcasted_iota(jnp.int32, (8, STORED), 0)
    layer_of = lax.broadcasted_iota(jnp.int32, (8, STORED), 1)
    wanted = jnp.where(row_of == 0, layer_ref[0], layer_ref[1])
    layer_pick = jnp.where((layer_of == wanted) & (row_of < LAYERS), 1.0, 0.0).astype(jnp.float32)

    def picked(table, columns):
        dot = functools.partial(
            jnp.dot, precision=lax.Precision.HIGHEST, preferred_element_type=jnp.float32
        )
        return dot(dot(layer_pick, table.astype(jnp.float32)), columns)

    blocks = 2 * FF // BLK
    block_of = lax.broadcasted_iota(jnp.int32, (blocks, 128), 0)
    to = lax.broadcasted_iota(jnp.int32, (blocks, 128), 1)
    source = me * BLOCKS + jnp.where(to < BLOCKS, to, FF // BLK + to - BLOCKS)
    pick_g = jnp.where((block_of == source) & (to < 2 * BLOCKS), 1.0, 0.0).astype(jnp.float32)
    head_of = lax.broadcasted_iota(jnp.int32, (NHEAD, 128), 0)
    to = lax.broadcasted_iota(jnp.int32, (NHEAD, 128), 1)
    pick_q = jnp.zeros((NHEAD, 128), jnp.float32)
    for s in range(SLOTS):
        hit = (head_of == slot_ref[me * SLOTS + s]) & (to == 2 * BLOCKS + s)
        pick_q = jnp.where(hit, 1.0, pick_q)
    expected = (picked(table_g[...], pick_g) + picked(table_q[...], pick_q)) * stored_unit

    others = pl.ds(0, N_DEV - 1)
    pltpu.make_async_copy(sum_recv.at[others], sum_recv.at[others], sum_sem.at[1]).wait()
    part_send[...] = jnp.sum(sum_recv[...], axis=0)
    part_recv[0] = part_send[...]
    for k in range(1, N_GRP):
        pltpu.make_async_remote_copy(
            src_ref=part_send,
            dst_ref=part_recv.at[k],
            send_sem=part_sem.at[0],
            recv_sem=part_sem.at[1],
            device_id={"grp": (grp + k) % N_GRP},
            device_id_type=MESH,
        ).start()
    parts = pl.ds(1, N_GRP - 1)
    pltpu.make_async_copy(part_recv.at[parts], part_recv.at[parts], part_sem.at[1]).wait()
    mismatch[...] = jnp.sum(part_recv[...], axis=0) - expected[:LAYERS]

    pltpu.make_async_copy(part_recv.at[parts], part_recv.at[parts], part_sem.at[0]).wait()
    pltpu.make_async_copy(sum_recv.at[others], sum_recv.at[others], sum_sem.at[0]).wait()
    for copy in own_copies:
        copy.wait()
    moved = pl.ds(0, (N_DEV - 1) * ROWS)
    for at in range(2):
        pltpu.make_async_copy(qkv_out.at[moved], qkv_out.at[moved], qkv_sem.at[at]).wait()
        pltpu.make_async_copy(gate_out.at[moved], gate_out.at[moved], gate_sem.at[at]).wait()


def body(qkv_weight, gate_up_weight, head_slot, layer_ids, stored_qkv, stored_gate_up):
    anywhere = pl.BlockSpec(memory_space=pl.ANY)
    scalars = pl.BlockSpec(memory_space=pltpu.SMEM)
    in_vmem = pl.BlockSpec(memory_space=pltpu.VMEM)
    total_rows = N_DEV * ROWS
    gate, qkv, mismatch = pl.pallas_call(
        kernel,
        out_shape=(
            jax.ShapeDtypeStruct((total_rows, LAYERS, 2 * WIDTH), jnp.bfloat16),
            jax.ShapeDtypeStruct((total_rows, LAYERS, QW), jnp.bfloat16),
            jax.ShapeDtypeStruct((LAYERS, 128), jnp.float32),
        ),
        in_specs=[anywhere, anywhere, scalars, scalars, anywhere, anywhere],
        out_specs=(anywhere, anywhere, in_vmem),
        scratch_shapes=[
            pltpu.VMEM((NHEAD, ROWS, LAYERS, HEAD_DIM), jnp.bfloat16),
            pltpu.VMEM((N_DEV, ROWS, LAYERS, QW), jnp.bfloat16),
            pltpu.VMEM((2, 2, ROWS, LAYERS, WIDTH), jnp.bfloat16),
            pltpu.VMEM((N_DEV, LAYERS, 128), jnp.float32),
            pltpu.VMEM((N_DEV, LAYERS, 128), jnp.float32),
            pltpu.VMEM((LAYERS, 128), jnp.float32),
            pltpu.VMEM((N_GRP, LAYERS, 128), jnp.float32),
            pltpu.VMEM((STORED, NHEAD), jnp.int32),
            pltpu.VMEM((STORED, 2 * FF // BLK), jnp.int32),
            pltpu.SemaphoreType.DMA((2,)),
            pltpu.SemaphoreType.DMA((2,)),
            pltpu.SemaphoreType.DMA((2,)),
            pltpu.SemaphoreType.DMA((2,)),
            pltpu.SemaphoreType.DMA((3,)),
            pltpu.SemaphoreType.DMA((2, 2)),
            pltpu.SemaphoreType.DMA((3,)),
        ],
        compiler_params=pltpu.CompilerParams(collective_id=0, has_side_effects=True),
        name="exchange",
    )(
        gate_up_weight.transpose(1, 0, 2),
        qkv_weight.transpose(1, 0, 2),
        head_slot,
        layer_ids,
        stored_qkv,
        stored_gate_up,
    )
    return (
        qkv.transpose(1, 0, 2),
        gate.transpose(1, 0, 2),
        mismatch[:, 2 * BLOCKS : 2 * BLOCKS + SLOTS],
        mismatch[:, : 2 * BLOCKS],
    )


def solution(mesh):
    placed = (P(None, ("grp", "dev"), None), P(None, ("grp", "dev"), None), P(), P(), P(), P())
    return jax.shard_map(
        body,
        mesh=mesh,
        in_specs=placed,
        out_specs=(P(None, "grp", "dev"), P(None, "grp", "dev"), P(None, "dev"), P(None, "dev")),
        check_vma=False,
    )
```

```python
import functools

import jax
import jax.numpy as jnp
from jax import lax
from jax.experimental import pallas as pl
from jax.experimental.pallas import tpu as pltpu
from jax.sharding import PartitionSpec as P

HEAD_DIM = 128
FF = 36864
STORED = 46
BLK = 128
NHEAD = 64
LAYERS = 2
ROWS = 36
N_DEV = 32
N_GRP = 4
WIDTH = FF // N_DEV
BLOCKS = WIDTH // BLK
SLOTS = NHEAD // N_DEV
QW = SLOTS * HEAD_DIM

stored_unit = 1.0 / 1024.0
MESH = pl.DeviceIdType.MESH

FAR_X = ((2, 1, 0, 1), (0, 1, 0, 1), (2, -1, 0, 1), (0, -1, 0, 1))
FAR_Y = ((1, 2, 1, 0), (-1, 0, 1, 0), (-1, 2, 1, 0), (1, 0, 1, 0))
DIAGONAL = ((1, 1, 1, 0), (-1, -1, 1, 0), (1, -1, 1, 0), (-1, 1, 1, 0))
OPPOSITE = ((2, 0, 0, 0), (0, 2, 0, 0), (2, 2, 0, 0))
ROUNDS = (FAR_X, FAR_Y, DIAGONAL, OPPOSITE)


def owner_at(me, offset, flip):
    dx, dy, mirror_x, mirror_y = offset
    x, y, core = me // 8, (me // 2) % 4, me % 2
    sign = 1 - 2 * core
    x = (x + (dx * sign if mirror_x else dx) + 4) % 4
    y = (y + (dy * sign if mirror_y else dy) + 4) % 4
    return (x * 4 + y) * 2 + (core + flip) % 2


def kernel(
    gate, qkv, slot_ref, layer_ref, stored_q, stored_g,
    gate_out, qkv_out, mismatch,
    gate_land, qkv_land,
    qkv_in, qkv_send, rows_in, sum_send, sum_recv, part_send, part_recv, part_total, part_land,
    table_q, table_g, gate_sem, gate_recv, qkv_sem, qkv_recv, sum_sem, part_sem, load_sem, table_sem,
):
    me = lax.axis_index("dev")
    grp = lax.axis_index("grp")

    load_tq = pltpu.make_async_copy(stored_q, table_q, table_sem.at[1])
    load_tg = pltpu.make_async_copy(stored_g, table_g, table_sem.at[2])

    def load_head(head, _):
        column = pl.ds(pl.multiple_of(head * HEAD_DIM, HEAD_DIM), HEAD_DIM)
        pltpu.make_async_copy(qkv.at[:, :, column], qkv_in.at[head], table_sem.at[0]).start()
        return 0

    lax.fori_loop(0, NHEAD, load_head, 0)
    load_tq.start()
    load_tg.start()

    barrier = pltpu.get_barrier_semaphore()

    def greet(k, _):
        pl.semaphore_signal(barrier, inc=1, device_id={"dev": (me + k) % N_DEV}, device_id_type=MESH)
        return 0

    lax.fori_loop(1, N_DEV, greet, 0)

    def greet_later(k, _):
        pl.semaphore_signal(barrier, inc=1, device_id={"grp": k}, device_id_type=MESH)
        return 0

    lax.fori_loop(grp + 1, N_GRP, greet_later, 0)
    pl.semaphore_wait(barrier, N_DEV - 1 + grp)

    own_rows = pl.ds(me * ROWS, ROWS)

    def send_gate(owner, p):
        pltpu.make_async_remote_copy(
            src_ref=gate.at[:, :, pl.ds(pl.multiple_of(p * FF + owner * WIDTH, BLK), WIDTH)],
            dst_ref=gate_land.at[own_rows, :, pl.ds(pl.multiple_of(p * WIDTH, BLK), WIDTH)],
            send_sem=gate_sem,
            recv_sem=gate_recv.at[me],
            device_id={"dev": owner},
            device_id_type=MESH,
        ).start()

    def send_qkv(owner):
        pltpu.make_async_remote_copy(
            src_ref=qkv_send.at[owner],
            dst_ref=qkv_land.at[own_rows],
            send_sem=qkv_sem,
            recv_sem=qkv_recv.at[me],
            device_id={"dev": owner},
            device_id_type=MESH,
        ).start()

    def gate_round(offsets):
        def step(i, _):
            for offset in offsets:
                send_gate(owner_at(me, offset, i % 2), i // 2)
            return 0

        lax.fori_loop(0, 4, step, 0)

    partner = owner_at(me, (0, 0, 0, 0), 1)
    for p in range(2):
        send_gate(partner, p)
    gate_round(ROUNDS[0])
    gate_round(ROUNDS[1])
    for p in range(2):
        pltpu.make_async_copy(
            gate.at[:, :, pl.ds(pl.multiple_of(p * FF + me * WIDTH, BLK), WIDTH)],
            gate_land.at[own_rows, :, pl.ds(p * WIDTH, WIDTH)],
            gate_recv.at[me],
        ).start()

    pltpu.make_async_copy(qkv_in, qkv_in, table_sem.at[0]).wait()

    def place(slot, _):
        part = qkv_in[slot_ref[slot]]
        column = pl.ds(pl.multiple_of((slot % SLOTS) * HEAD_DIM, HEAD_DIM), HEAD_DIM)
        qkv_send[slot // SLOTS, :, :, column] = part
        return 0

    lax.fori_loop(0, NHEAD, place, 0)

    def load(owner, slot):
        return [
            pltpu.make_async_copy(
                gate.at[:, :, pl.ds(pl.multiple_of(p * FF + owner * WIDTH, BLK), WIDTH)],
                rows_in.at[slot, p],
                load_sem.at[slot, p],
            )
            for p in range(2)
        ]

    lane = lax.broadcasted_iota(jnp.int32, (LAYERS, 128), 1)

    def block_total(values, at, total):
        rows = jnp.sum(values.astype(jnp.float32), axis=0)
        return jnp.where(lane == at, jnp.sum(rows, axis=1, keepdims=True), total)

    for copy in load(0, 0):
        copy.start()

    def add_up(owner, _):
        slot = owner % 2

        @pl.when(owner + 1 < N_DEV)
        def _():
            for copy in load(owner + 1, 1 - slot):
                copy.start()

        for copy in load(owner, slot):
            copy.wait()
        total = jnp.zeros((LAYERS, 128), jnp.float32)
        for p in range(2):
            for b in range(BLOCKS):
                total = block_total(rows_in[slot, p, :, :, b * BLK : (b + 1) * BLK], p * BLOCKS + b, total)
        for s in range(SLOTS):
            total = block_total(
                qkv_send[owner, :, :, s * HEAD_DIM : (s + 1) * HEAD_DIM], 2 * BLOCKS + s, total
            )
        sum_send[owner] = total
        return 0

    lax.fori_loop(0, N_DEV, add_up, 0)

    def send_qkv_round(offsets, flip):
        for offset in offsets:
            send_qkv(owner_at(me, offset, flip))

    def small_sends(i, _):
        owner = (me + i) % N_DEV
        pltpu.make_async_remote_copy(
            src_ref=sum_send.at[owner],
            dst_ref=sum_recv.at[me],
            send_sem=sum_sem.at[0],
            recv_sem=sum_sem.at[1],
            device_id={"dev": owner},
            device_id_type=MESH,
        ).start()
        return 0

    lax.fori_loop(1, N_DEV, small_sends, 0)
    send_qkv(partner)

    def qkv_sends(flip, _):
        for offsets in ROUNDS:
            send_qkv_round(offsets, flip)
        return 0

    lax.fori_loop(0, 2, qkv_sends, 0)
    gate_round(ROUNDS[2])
    gate_round(ROUNDS[3])

    sum_recv[me] = sum_send[me]
    qkv_land[own_rows] = qkv_send[me]

    load_tq.wait()
    load_tg.wait()
    row_of = lax.broadcasted_iota(jnp.int32, (8, STORED), 0)
    layer_of = lax.broadcasted_iota(jnp.int32, (8, STORED), 1)
    wanted = jnp.where(row_of == 0, layer_ref[0], layer_ref[1])
    layer_pick = jnp.where((layer_of == wanted) & (row_of < LAYERS), 1.0, 0.0).astype(jnp.float32)

    def picked(table, columns):
        dot = functools.partial(
            jnp.dot, precision=lax.Precision.HIGHEST, preferred_element_type=jnp.float32
        )
        return dot(dot(layer_pick, table.astype(jnp.float32)), columns)

    blocks = 2 * FF // BLK
    block_of = lax.broadcasted_iota(jnp.int32, (blocks, 128), 0)
    to = lax.broadcasted_iota(jnp.int32, (blocks, 128), 1)
    source = me * BLOCKS + jnp.where(to < BLOCKS, to, FF // BLK + to - BLOCKS)
    pick_g = jnp.where((block_of == source) & (to < 2 * BLOCKS), 1.0, 0.0).astype(jnp.float32)
    head_of = lax.broadcasted_iota(jnp.int32, (NHEAD, 128), 0)
    to = lax.broadcasted_iota(jnp.int32, (NHEAD, 128), 1)
    pick_q = jnp.zeros((NHEAD, 128), jnp.float32)
    for s in range(SLOTS):
        hit = (head_of == slot_ref[me * SLOTS + s]) & (to == 2 * BLOCKS + s)
        pick_q = jnp.where(hit, 1.0, pick_q)
    expected = (picked(table_g[...], pick_g) + picked(table_q[...], pick_q)) * stored_unit

    def take_apart(land, out, chip, column):
        start = pl.multiple_of(chip * 2 * ROWS, 8)
        rows = land[pl.ds(start, 2 * ROWS), :, column].reshape(2 * ROWS // 8, 8, LAYERS, BLK)
        rows = jnp.swapaxes(rows, 1, 2)
        for i in range(2 * ROWS // 8):
            for layer in range(LAYERS):
                out[layer, pl.ds(pl.multiple_of(start + 8 * i, 8), 8), column] = rows[i, layer]

    def settle(land, out, landed, width, offset, only=None):
        x, y = me // 8, (me // 2) % 4
        chip = (x + offset[0] + 4) % 4 * 4 + (y + offset[1] + 4) % 4
        for core in range(2):
            source = chip * 2 + core
            block = land.at[pl.ds(source * ROWS, ROWS)]
            wait = pltpu.make_async_copy(block, block, landed.at[source]).wait
            if only is None:
                wait()
            else:
                pl.when(source != me)(wait)

        def step(i, _):
            take_apart(land, out, chip, pl.ds(pl.multiple_of(i * BLK, BLK), BLK))
            return 0

        lax.fori_loop(0, width // BLK, step, 0)

    def settle_gate(offsets):
        for offset in offsets:
            settle(gate_land, gate_out, gate_recv, 2 * WIDTH, offset)

    here = ((0, 0),)
    settle_gate(here)
    settle_gate(ROUNDS[0])
    settle_gate(ROUNDS[1])

    others = pl.ds(0, N_DEV - 1)
    pltpu.make_async_copy(sum_recv.at[others], sum_recv.at[others], sum_sem.at[1]).wait()
    part_send[...] = jnp.sum(sum_recv[...], axis=0)
    to_first = pltpu.make_async_remote_copy(
        src_ref=part_send,
        dst_ref=part_recv.at[grp],
        send_sem=part_sem.at[0],
        recv_sem=part_sem.at[1],
        device_id={"grp": 0},
        device_id_type=MESH,
    )

    @pl.when(grp > 0)
    def _():
        to_first.start()

    settle(qkv_land, qkv_out, qkv_recv, QW, here[0], only="others")
    for offsets in ROUNDS:
        for offset in offsets:
            settle(qkv_land, qkv_out, qkv_recv, QW, offset)
    parts = pl.ds(1, N_GRP - 1)
    from_others = part_recv.at[parts]

    def total_to(k):
        return pltpu.make_async_remote_copy(
            src_ref=part_total,
            dst_ref=part_land,
            send_sem=part_sem.at[2],
            recv_sem=part_sem.at[3],
            device_id={"grp": k},
            device_id_type=MESH,
        )

    @pl.when(grp == 0)
    def _():
        part_recv[0] = part_send[...]
        pltpu.make_async_copy(from_others, from_others, part_sem.at[1]).wait()
        total = jnp.sum(part_recv[...], axis=0)
        part_total[...] = total
        mismatch[...] = total - expected[:LAYERS]
        for k in range(1, N_GRP):
            total_to(k).start()

    settle_gate(ROUNDS[2])
    settle_gate(ROUNDS[3])

    @pl.when(grp > 0)
    def _():
        pltpu.make_async_copy(part_land, part_land, part_sem.at[3]).wait()
        mismatch[...] = part_land[...] - expected[:LAYERS]
        to_first.wait_send()

    @pl.when(grp == 0)
    def _():
        pltpu.make_async_copy(from_others, from_others, part_sem.at[2]).wait()

    pltpu.make_async_copy(sum_recv.at[others], sum_recv.at[others], sum_sem.at[0]).wait()
    moved = pl.ds(0, (N_DEV - 1) * ROWS)
    pltpu.make_async_copy(qkv_land.at[moved], qkv_land.at[moved], qkv_sem).wait()
    pltpu.make_async_copy(gate_land.at[moved], gate_land.at[moved], gate_sem).wait()


def body(qkv_weight, gate_up_weight, head_slot, layer_ids, stored_qkv, stored_gate_up):
    anywhere = pl.BlockSpec(memory_space=pl.ANY)
    scalars = pl.BlockSpec(memory_space=pltpu.SMEM)
    in_vmem = pl.BlockSpec(memory_space=pltpu.VMEM)
    total_rows = N_DEV * ROWS
    gate, qkv, mismatch = pl.pallas_call(
        kernel,
        out_shape=(
            pltpu.VMEM((LAYERS, total_rows, 2 * WIDTH), jnp.bfloat16),
            pltpu.VMEM((LAYERS, total_rows, QW), jnp.bfloat16),
            pltpu.VMEM((LAYERS, 128), jnp.float32),
        ),
        in_specs=[anywhere, anywhere, scalars, scalars, anywhere, anywhere],
        out_specs=(in_vmem, in_vmem, in_vmem),
        scratch_shapes=[
            pltpu.VMEM((total_rows, LAYERS, 2 * WIDTH), jnp.bfloat16),
            pltpu.VMEM((total_rows, LAYERS, QW), jnp.bfloat16),
            pltpu.VMEM((NHEAD, ROWS, LAYERS, HEAD_DIM), jnp.bfloat16),
            pltpu.VMEM((N_DEV, ROWS, LAYERS, QW), jnp.bfloat16),
            pltpu.VMEM((2, 2, ROWS, LAYERS, WIDTH), jnp.bfloat16),
            pltpu.VMEM((N_DEV, LAYERS, 128), jnp.float32),
            pltpu.VMEM((N_DEV, LAYERS, 128), jnp.float32),
            pltpu.VMEM((LAYERS, 128), jnp.float32),
            pltpu.VMEM((N_GRP, LAYERS, 128), jnp.float32),
            pltpu.VMEM((LAYERS, 128), jnp.float32),
            pltpu.VMEM((LAYERS, 128), jnp.float32),
            pltpu.VMEM((STORED, NHEAD), jnp.int32),
            pltpu.VMEM((STORED, 2 * FF // BLK), jnp.int32),
            pltpu.SemaphoreType.DMA,
            pltpu.SemaphoreType.DMA((N_DEV,)),
            pltpu.SemaphoreType.DMA,
            pltpu.SemaphoreType.DMA((N_DEV,)),
            pltpu.SemaphoreType.DMA((2,)),
            pltpu.SemaphoreType.DMA((4,)),
            pltpu.SemaphoreType.DMA((2, 2)),
            pltpu.SemaphoreType.DMA((3,)),
        ],
        compiler_params=pltpu.CompilerParams(
            collective_id=0, has_side_effects=True, vmem_limit_bytes=50 << 20
        ),
        name="exchange",
    )(
        gate_up_weight.transpose(1, 0, 2),
        qkv_weight.transpose(1, 0, 2),
        head_slot,
        layer_ids,
        stored_qkv,
        stored_gate_up,
    )
    return (
        qkv,
        gate,
        mismatch[:, 2 * BLOCKS : 2 * BLOCKS + SLOTS],
        mismatch[:, : 2 * BLOCKS],
    )


def solution(mesh):
    placed = (P(None, ("grp", "dev"), None), P(None, ("grp", "dev"), None), P(), P(), P(), P())
    return jax.shard_map(
        body,
        mesh=mesh,
        in_specs=placed,
        out_specs=(P(None, "grp", "dev"), P(None, "grp", "dev"), P(None, "dev"), P(None, "dev")),
        check_vma=False,
    )
```

```python
import functools

import jax
import jax.numpy as jnp
from jax import lax
from jax.experimental import pallas as pl
from jax.experimental.pallas import tpu as pltpu
from jax.sharding import PartitionSpec as P

HEAD_DIM = 128
FF = 36864
STORED = 46
BLK = 128
NHEAD = 64
LAYERS = 2
ROWS = 36
N_DEV = 32
N_GRP = 4
WIDTH = FF // N_DEV
BLOCKS = WIDTH // BLK
SLOTS = NHEAD // N_DEV
QW = SLOTS * HEAD_DIM
PIECES = 4

stored_unit = 1.0 / 1024.0
MESH = pl.DeviceIdType.MESH

FAR_X = ((2, 1, 0, 1), (0, 1, 0, 1), (2, -1, 0, 1), (0, -1, 0, 1))
FAR_Y = ((1, 2, 1, 0), (-1, 0, 1, 0), (-1, 2, 1, 0), (1, 0, 1, 0))
DIAGONAL = ((1, 1, 1, 0), (-1, -1, 1, 0), (1, -1, 1, 0), (-1, 1, 1, 0))
OPPOSITE = ((2, 0, 0, 0), (0, 2, 0, 0), (2, 2, 0, 0))
ROUNDS = (FAR_X, OPPOSITE, FAR_Y, DIAGONAL)


def owner_at(me, offset, flip):
    dx, dy, mirror_x, mirror_y = offset
    x, y, core = me // 8, (me // 2) % 4, me % 2
    sign = 1 - 2 * core
    x = (x + (dx * sign if mirror_x else dx) + 4) % 4
    y = (y + (dy * sign if mirror_y else dy) + 4) % 4
    return (x * 4 + y) * 2 + (core + flip) % 2


def kernel(
    gate, qkv, head_slot, layer_ids, stored_q, stored_g,
    gate_out, qkv_out, qkv_mismatch, gate_mismatch,
    gate_land, qkv_land,
    qkv_in, qkv_send, rows_in, sum_send, sum_recv, part_send, part_recv, part_total, part_land,
    slot_ref, layer_ref, table_q, table_g, gate_sem, gate_recv, qkv_sem, qkv_recv, sum_sem, part_sem, load_sem, table_sem,
):
    me = lax.axis_index("dev")
    grp = lax.axis_index("grp")

    barrier = pltpu.get_barrier_semaphore()

    def greet(k, _):
        pl.semaphore_signal(barrier, inc=1, device_id={"dev": (me + k) % N_DEV}, device_id_type=MESH)
        return 0

    lax.fori_loop(1, N_DEV, greet, 0)

    def greet_later(k, _):
        pl.semaphore_signal(barrier, inc=1, device_id={"grp": k}, device_id_type=MESH)
        return 0

    lax.fori_loop(grp + 1, N_GRP, greet_later, 0)
    pl.semaphore_wait(barrier, N_DEV - 1 + grp)

    own_rows = pl.ds(me * ROWS, ROWS)

    def send_gate(owner, p):
        pltpu.make_async_remote_copy(
            src_ref=gate.at[:, :, pl.ds(pl.multiple_of(p * FF + owner * WIDTH, BLK), WIDTH)],
            dst_ref=gate_land.at[own_rows, :, pl.ds(pl.multiple_of(p * WIDTH, BLK), WIDTH)],
            send_sem=gate_sem,
            recv_sem=gate_recv.at[me],
            device_id={"dev": owner},
            device_id_type=MESH,
        ).start()

    def send_qkv(owner):
        pltpu.make_async_remote_copy(
            src_ref=qkv_send.at[owner],
            dst_ref=qkv_land.at[own_rows],
            send_sem=qkv_sem,
            recv_sem=qkv_recv.at[me],
            device_id={"dev": owner},
            device_id_type=MESH,
        ).start()

    def gate_round(offsets):
        def step(i, _):
            for offset in offsets:
                send_gate(owner_at(me, offset, i % 2), i // 2)
            return 0

        lax.fori_loop(0, 4, step, 0)

    partner = owner_at(me, (0, 0, 0, 0), 1)
    for p in range(2):
        send_gate(partner, p)
    gate_round(ROUNDS[0])
    gate_round(ROUNDS[1])
    for p in range(2):
        pltpu.make_async_copy(
            gate.at[:, :, pl.ds(pl.multiple_of(p * FF + me * WIDTH, BLK), WIDTH)],
            gate_land.at[own_rows, :, pl.ds(p * WIDTH, WIDTH)],
            gate_recv.at[me],
        ).start()

    fetches = [
        pltpu.make_async_copy(source, target, table_sem.at[1 + i])
        for i, (source, target) in enumerate(
            ((head_slot, slot_ref), (layer_ids, layer_ref), (stored_q, table_q), (stored_g, table_g))
        )
    ]
    for fetch in fetches:
        fetch.start()

    def load_head(head, _):
        column = pl.ds(pl.multiple_of(head * HEAD_DIM, HEAD_DIM), HEAD_DIM)
        pltpu.make_async_copy(qkv.at[:, :, column], qkv_in.at[head], table_sem.at[0]).start()
        return 0

    lax.fori_loop(0, NHEAD, load_head, 0)
    for fetch in fetches:
        fetch.wait()
    pltpu.make_async_copy(qkv_in, qkv_in, table_sem.at[0]).wait()

    def place(slot, _):
        part = qkv_in[slot_ref[slot]]
        column = pl.ds(pl.multiple_of((slot % SLOTS) * HEAD_DIM, HEAD_DIM), HEAD_DIM)
        qkv_send[slot // SLOTS, :, :, column] = part
        return 0

    lax.fori_loop(0, NHEAD, place, 0)

    def load(owner, slot):
        return [
            pltpu.make_async_copy(
                gate.at[:, :, pl.ds(pl.multiple_of(p * FF + owner * WIDTH, BLK), WIDTH)],
                rows_in.at[slot, p],
                load_sem.at[slot, p],
            )
            for p in range(2)
        ]

    lane = lax.broadcasted_iota(jnp.int32, (LAYERS, 128), 1)

    def block_total(values, at, total):
        rows = jnp.sum(values.astype(jnp.float32), axis=0)
        return jnp.where(lane == at, jnp.sum(rows, axis=1, keepdims=True), total)

    for copy in load(0, 0):
        copy.start()

    def add_up(owner, _):
        slot = owner % 2

        @pl.when(owner + 1 < N_DEV)
        def _():
            for copy in load(owner + 1, 1 - slot):
                copy.start()

        for copy in load(owner, slot):
            copy.wait()
        total = jnp.zeros((LAYERS, 128), jnp.float32)
        for p in range(2):
            for b in range(BLOCKS):
                total = block_total(rows_in[slot, p, :, :, b * BLK : (b + 1) * BLK], p * BLOCKS + b, total)
        for s in range(SLOTS):
            total = block_total(
                qkv_send[owner, :, :, s * HEAD_DIM : (s + 1) * HEAD_DIM], 2 * BLOCKS + s, total
            )
        sum_send[owner] = total
        return 0

    lax.fori_loop(0, N_DEV, add_up, 0)

    def send_qkv_round(offsets, flip):
        for offset in offsets:
            send_qkv(owner_at(me, offset, flip))

    def small_sends(i, _):
        owner = (me + i) % N_DEV
        pltpu.make_async_remote_copy(
            src_ref=sum_send.at[owner],
            dst_ref=sum_recv.at[me],
            send_sem=sum_sem.at[0],
            recv_sem=sum_sem.at[1],
            device_id={"dev": owner},
            device_id_type=MESH,
        ).start()
        return 0

    lax.fori_loop(1, N_DEV, small_sends, 0)
    send_qkv(partner)

    def qkv_sends(flip, _):
        for offsets in ROUNDS:
            send_qkv_round(offsets, flip)
        return 0

    lax.fori_loop(0, 2, qkv_sends, 0)
    gate_round(ROUNDS[2])
    gate_round(ROUNDS[3])

    sum_recv[me] = sum_send[me]
    qkv_land[own_rows] = qkv_send[me]

    row_of = lax.broadcasted_iota(jnp.int32, (8, STORED), 0)
    layer_of = lax.broadcasted_iota(jnp.int32, (8, STORED), 1)
    wanted = jnp.where(row_of == 0, layer_ref[0], layer_ref[1])
    layer_pick = jnp.where((layer_of == wanted) & (row_of < LAYERS), 1.0, 0.0).astype(jnp.float32)

    def picked(table, columns):
        dot = functools.partial(
            jnp.dot, precision=lax.Precision.HIGHEST, preferred_element_type=jnp.float32
        )
        return dot(dot(layer_pick, table.astype(jnp.float32)), columns)

    blocks = 2 * FF // BLK
    block_of = lax.broadcasted_iota(jnp.int32, (blocks, 128), 0)
    to = lax.broadcasted_iota(jnp.int32, (blocks, 128), 1)
    source = me * BLOCKS + jnp.where(to < BLOCKS, to, FF // BLK + to - BLOCKS)
    pick_g = jnp.where((block_of == source) & (to < 2 * BLOCKS), 1.0, 0.0).astype(jnp.float32)
    head_of = lax.broadcasted_iota(jnp.int32, (NHEAD, 128), 0)
    to = lax.broadcasted_iota(jnp.int32, (NHEAD, 128), 1)
    pick_q = jnp.zeros((NHEAD, 128), jnp.float32)
    for s in range(SLOTS):
        hit = (head_of == slot_ref[me * SLOTS + s]) & (to == 2 * BLOCKS + s)
        pick_q = jnp.where(hit, 1.0, pick_q)
    expected = (picked(table_g[...], pick_g) + picked(table_q[...], pick_q)) * stored_unit

    def take_apart(land, out, chip, column):
        start = pl.multiple_of(chip * 2 * ROWS, 8)
        rows = land[pl.ds(start, 2 * ROWS), :, column].reshape(2 * ROWS // 8, 8, LAYERS, BLK)
        rows = jnp.swapaxes(rows, 1, 2)
        for i in range(2 * ROWS // 8):
            for layer in range(LAYERS):
                out[layer, pl.ds(pl.multiple_of(start + 8 * i, 8), 8), column] = rows[i, layer]

    def settle(land, out, landed, width, offset, only=None):
        x, y = me // 8, (me // 2) % 4
        chip = (x + offset[0] + 4) % 4 * 4 + (y + offset[1] + 4) % 4
        for core in range(2):
            source = chip * 2 + core
            block = land.at[pl.ds(source * ROWS, ROWS)]
            wait = pltpu.make_async_copy(block, block, landed.at[source]).wait
            if only is None:
                wait()
            else:
                pl.when(source != me)(wait)

        def step(i, _):
            take_apart(land, out, chip, pl.ds(pl.multiple_of(i * BLK, BLK), BLK))
            return 0

        lax.fori_loop(0, width // BLK, step, 0)

    def settle_gate(offsets):
        for offset in offsets:
            settle(gate_land, gate_out, gate_recv, 2 * WIDTH, offset)

    here = ((0, 0),)
    settle_gate(here)
    settle_gate(ROUNDS[0])
    settle_gate(ROUNDS[1])

    others = pl.ds(0, N_DEV - 1)
    pltpu.make_async_copy(sum_recv.at[others], sum_recv.at[others], sum_sem.at[1]).wait()
    part_send[...] = jnp.sum(sum_recv[...], axis=0)
    to_first = pltpu.make_async_remote_copy(
        src_ref=part_send,
        dst_ref=part_recv.at[grp],
        send_sem=part_sem.at[0],
        recv_sem=part_sem.at[1],
        device_id={"grp": 0},
        device_id_type=MESH,
    )

    @pl.when(grp > 0)
    def _():
        to_first.start()

    settle(qkv_land, qkv_out, qkv_recv, QW, here[0], only="others")
    for offsets in ROUNDS:
        for offset in offsets:
            settle(qkv_land, qkv_out, qkv_recv, QW, offset)
    parts = pl.ds(1, N_GRP - 1)
    from_others = part_recv.at[parts]

    def give(total):
        difference = total - expected[:LAYERS]
        gate_mismatch[...] = difference[:, : 2 * BLOCKS]
        qkv_mismatch[...] = difference[:, 2 * BLOCKS : 2 * BLOCKS + SLOTS]

    def total_to(k):
        return pltpu.make_async_remote_copy(
            src_ref=part_total,
            dst_ref=part_land,
            send_sem=part_sem.at[2],
            recv_sem=part_sem.at[3],
            device_id={"grp": k},
            device_id_type=MESH,
        )

    @pl.when(grp == 0)
    def _():
        part_recv[0] = part_send[...]
        pltpu.make_async_copy(from_others, from_others, part_sem.at[1]).wait()
        total = jnp.sum(part_recv[...], axis=0)
        part_total[...] = total
        give(total)
        for k in range(1, N_GRP):
            total_to(k).start()

    settle_gate(ROUNDS[2])
    settle_gate(ROUNDS[3])

    @pl.when(grp > 0)
    def _():
        pltpu.make_async_copy(part_land, part_land, part_sem.at[3]).wait()
        give(part_land[...])
        to_first.wait_send()

    @pl.when(grp == 0)
    def _():
        pltpu.make_async_copy(from_others, from_others, part_sem.at[2]).wait()

    pltpu.make_async_copy(sum_recv.at[others], sum_recv.at[others], sum_sem.at[0]).wait()
    moved = pl.ds(0, (N_DEV - 1) * ROWS)
    pltpu.make_async_copy(qkv_land.at[moved], qkv_land.at[moved], qkv_sem).wait()
    pltpu.make_async_copy(gate_land.at[moved], gate_land.at[moved], gate_sem).wait()


def put_out(gate, qkv, qkv_mismatch, gate_mismatch, gate_out, qkv_out, qkv_m_out, gate_m_out, sem):
    height = N_DEV * ROWS // PIECES
    pairs = [
        (gate.at[layer, pl.ds(k * height, height)], gate_out.at[layer, pl.ds(k * height, height)])
        for layer in range(LAYERS)
        for k in range(PIECES)
    ]
    pairs += [(qkv, qkv_out), (qkv_mismatch, qkv_m_out), (gate_mismatch, gate_m_out)]
    copies = [pltpu.make_async_copy(a, b, sem.at[i]) for i, (a, b) in enumerate(pairs)]
    for copy in copies:
        copy.start()
    for copy in copies:
        copy.wait()


def body(qkv_weight, gate_up_weight, head_slot, layer_ids, stored_qkv, stored_gate_up):
    anywhere = pl.BlockSpec(memory_space=pl.ANY)
    in_vmem = pl.BlockSpec(memory_space=pltpu.VMEM)
    total_rows = N_DEV * ROWS
    landed = pl.pallas_call(
        kernel,
        out_shape=(
            pltpu.VMEM((LAYERS, total_rows, 2 * WIDTH), jnp.bfloat16),
            pltpu.VMEM((LAYERS, total_rows, QW), jnp.bfloat16),
            pltpu.VMEM((LAYERS, SLOTS), jnp.float32),
            pltpu.VMEM((LAYERS, 2 * BLOCKS), jnp.float32),
        ),
        in_specs=[anywhere] * 6,
        out_specs=(in_vmem,) * 4,
        scratch_shapes=[
            pltpu.VMEM((total_rows, LAYERS, 2 * WIDTH), jnp.bfloat16),
            pltpu.VMEM((total_rows, LAYERS, QW), jnp.bfloat16),
            pltpu.VMEM((NHEAD, ROWS, LAYERS, HEAD_DIM), jnp.bfloat16),
            pltpu.VMEM((N_DEV, ROWS, LAYERS, QW), jnp.bfloat16),
            pltpu.VMEM((2, 2, ROWS, LAYERS, WIDTH), jnp.bfloat16),
            pltpu.VMEM((N_DEV, LAYERS, 128), jnp.float32),
            pltpu.VMEM((N_DEV, LAYERS, 128), jnp.float32),
            pltpu.VMEM((LAYERS, 128), jnp.float32),
            pltpu.VMEM((N_GRP, LAYERS, 128), jnp.float32),
            pltpu.VMEM((LAYERS, 128), jnp.float32),
            pltpu.VMEM((LAYERS, 128), jnp.float32),
            pltpu.SMEM((NHEAD,), jnp.int32),
            pltpu.SMEM((LAYERS,), jnp.int32),
            pltpu.VMEM((STORED, NHEAD), jnp.int32),
            pltpu.VMEM((STORED, 2 * FF // BLK), jnp.int32),
            pltpu.SemaphoreType.DMA,
            pltpu.SemaphoreType.DMA((N_DEV,)),
            pltpu.SemaphoreType.DMA,
            pltpu.SemaphoreType.DMA((N_DEV,)),
            pltpu.SemaphoreType.DMA((2,)),
            pltpu.SemaphoreType.DMA((4,)),
            pltpu.SemaphoreType.DMA((2, 2)),
            pltpu.SemaphoreType.DMA((5,)),
        ],
        compiler_params=pltpu.CompilerParams(
            collective_id=0, has_side_effects=True, vmem_limit_bytes=50 << 20
        ),
        name="exchange",
    )(
        gate_up_weight.transpose(1, 0, 2),
        qkv_weight.transpose(1, 0, 2),
        head_slot,
        layer_ids,
        stored_qkv,
        stored_gate_up,
    )
    served_gate, served_qkv, qkv_mismatch, gate_mismatch = pl.pallas_call(
        put_out,
        out_shape=tuple(jax.ShapeDtypeStruct(a.shape, a.dtype) for a in landed),
        in_specs=[in_vmem] * 4,
        out_specs=(anywhere,) * 4,
        scratch_shapes=[pltpu.SemaphoreType.DMA((LAYERS * PIECES + 3,))],
        compiler_params=pltpu.CompilerParams(vmem_limit_bytes=1 << 20),
        name="put_out",
    )(*landed)
    return served_qkv, served_gate, qkv_mismatch, gate_mismatch


def solution(mesh):
    placed = (P(None, ("grp", "dev"), None), P(None, ("grp", "dev"), None), P(), P(), P(), P())
    return jax.shard_map(
        body,
        mesh=mesh,
        in_specs=placed,
        out_specs=(P(None, "grp", "dev"), P(None, "grp", "dev"), P(None, "dev"), P(None, "dev")),
        check_vma=False,
    )
```

```python
import functools

import jax
import jax.numpy as jnp
from jax import lax
from jax.experimental import pallas as pl
from jax.experimental.pallas import tpu as pltpu
from jax.sharding import PartitionSpec as P

HEAD_DIM = 128
FF = 36864
STORED = 46
BLK = 128
NHEAD = 64
LAYERS = 2
ROWS = 36
N_DEV = 32
N_GRP = 4
WIDTH = FF // N_DEV
BLOCKS = WIDTH // BLK
SLOTS = NHEAD // N_DEV
QW = SLOTS * HEAD_DIM
PIECES = 4

stored_unit = 1.0 / 1024.0
MESH = pl.DeviceIdType.MESH

FAR_X = ((2, 1, 0, 1), (0, 1, 0, 1), (2, -1, 0, 1), (0, -1, 0, 1))
FAR_Y = ((1, 2, 1, 0), (-1, 0, 1, 0), (-1, 2, 1, 0), (1, 0, 1, 0))
DIAGONAL = ((1, 1, 0, 0), (-1, -1, 0, 0))
ANTIDIAGONAL = ((1, -1, 0, 0), (-1, 1, 0, 0))
OPPOSITE = ((2, 0, 0, 0), (0, 2, 0, 0), (2, 2, 0, 0))
ROUNDS = (FAR_X, OPPOSITE, FAR_Y, DIAGONAL, ANTIDIAGONAL)


FAR_FIRST = sorted(range(1, N_DEV), key=lambda k: -(min(k // 8, 4 - k // 8) + min(k // 2 % 4, 4 - k // 2 % 4)))


def owner_at(me, offset, flip):
    dx, dy, mirror_x, mirror_y = offset
    x, y, core = me // 8, (me // 2) % 4, me % 2
    sign = 1 - 2 * core
    x = (x + (dx * sign if mirror_x else dx) + 4) % 4
    y = (y + (dy * sign if mirror_y else dy) + 4) % 4
    return (x * 4 + y) * 2 + (core + flip) % 2


def kernel(
    gate, qkv, head_slot, layer_ids, stored_q, stored_g,
    gate_out, qkv_out, qkv_mismatch, gate_mismatch,
    gate_land, qkv_land,
    qkv_in, qkv_send, rows_in, sum_send, sum_recv, part_send, part_recv, part_total, part_land,
    slot_ref, layer_ref, table_q, table_g, gate_sem, gate_recv, qkv_sem, qkv_recv, sum_sem, part_sem, load_sem, table_sem,
):
    me = lax.axis_index("dev")
    grp = lax.axis_index("grp")

    barrier = pltpu.get_barrier_semaphore()

    for k in FAR_FIRST:
        pl.semaphore_signal(barrier, inc=1, device_id={"dev": (me + k) % N_DEV}, device_id_type=MESH)

    def greet_later(k, _):
        pl.semaphore_signal(barrier, inc=1, device_id={"grp": k}, device_id_type=MESH)
        return 0

    lax.fori_loop(grp + 1, N_GRP, greet_later, 0)
    pl.semaphore_wait(barrier, N_DEV - 1 + grp)

    own_rows = pl.ds(me * ROWS, ROWS)

    def send_gate(owner, p):
        pltpu.make_async_remote_copy(
            src_ref=gate.at[:, :, pl.ds(pl.multiple_of(p * FF + owner * WIDTH, BLK), WIDTH)],
            dst_ref=gate_land.at[own_rows, :, pl.ds(pl.multiple_of(p * WIDTH, BLK), WIDTH)],
            send_sem=gate_sem,
            recv_sem=gate_recv.at[me, p],
            device_id={"dev": owner},
            device_id_type=MESH,
        ).start()

    def send_qkv(owner):
        pltpu.make_async_remote_copy(
            src_ref=qkv_send.at[owner],
            dst_ref=qkv_land.at[own_rows],
            send_sem=qkv_sem,
            recv_sem=qkv_recv.at[me],
            device_id={"dev": owner},
            device_id_type=MESH,
        ).start()

    def gate_round(offsets):
        def step(i, _):
            for offset in offsets:
                send_gate(owner_at(me, offset, i % 2), i // 2)
            return 0

        lax.fori_loop(0, 4, step, 0)

    partner = owner_at(me, (0, 0, 0, 0), 1)
    for p in range(2):
        send_gate(partner, p)
    gate_round(ROUNDS[0])
    gate_round(ROUNDS[1])
    for p in range(2):
        pltpu.make_async_copy(
            gate.at[:, :, pl.ds(pl.multiple_of(p * FF + me * WIDTH, BLK), WIDTH)],
            gate_land.at[own_rows, :, pl.ds(p * WIDTH, WIDTH)],
            gate_recv.at[me, p],
        ).start()

    fetches = [
        pltpu.make_async_copy(source, target, table_sem.at[1 + i])
        for i, (source, target) in enumerate(
            ((head_slot, slot_ref), (layer_ids, layer_ref), (stored_q, table_q), (stored_g, table_g))
        )
    ]
    for fetch in fetches:
        fetch.start()

    def load_head(head, _):
        column = pl.ds(pl.multiple_of(head * HEAD_DIM, HEAD_DIM), HEAD_DIM)
        pltpu.make_async_copy(qkv.at[:, :, column], qkv_in.at[head], table_sem.at[0]).start()
        return 0

    lax.fori_loop(0, NHEAD, load_head, 0)
    for fetch in fetches:
        fetch.wait()
    pltpu.make_async_copy(qkv_in, qkv_in, table_sem.at[0]).wait()

    def place(slot, _):
        part = qkv_in[slot_ref[slot]]
        column = pl.ds(pl.multiple_of((slot % SLOTS) * HEAD_DIM, HEAD_DIM), HEAD_DIM)
        qkv_send[slot // SLOTS, :, :, column] = part
        return 0

    lax.fori_loop(0, NHEAD, place, 0)

    def load(owner, slot):
        return [
            pltpu.make_async_copy(
                gate.at[:, :, pl.ds(pl.multiple_of(p * FF + owner * WIDTH, BLK), WIDTH)],
                rows_in.at[slot, p],
                load_sem.at[slot, p],
            )
            for p in range(2)
        ]

    lane = lax.broadcasted_iota(jnp.int32, (LAYERS, 128), 1)

    def block_total(values, at, total):
        rows = jnp.sum(values.astype(jnp.float32), axis=0)
        return jnp.where(lane == at, jnp.sum(rows, axis=1, keepdims=True), total)

    for copy in load(0, 0):
        copy.start()

    def add_up(owner, _):
        slot = owner % 2

        @pl.when(owner + 1 < N_DEV)
        def _():
            for copy in load(owner + 1, 1 - slot):
                copy.start()

        for copy in load(owner, slot):
            copy.wait()
        total = jnp.zeros((LAYERS, 128), jnp.float32)
        for p in range(2):
            for b in range(BLOCKS):
                total = block_total(rows_in[slot, p, :, :, b * BLK : (b + 1) * BLK], p * BLOCKS + b, total)
        for s in range(SLOTS):
            total = block_total(
                qkv_send[owner, :, :, s * HEAD_DIM : (s + 1) * HEAD_DIM], 2 * BLOCKS + s, total
            )
        sum_send[owner] = total
        return 0

    lax.fori_loop(0, N_DEV, add_up, 0)

    def send_qkv_round(offsets, flip):
        for offset in offsets:
            send_qkv(owner_at(me, offset, flip))

    def small_sends(i, _):
        owner = (me + i) % N_DEV
        pltpu.make_async_remote_copy(
            src_ref=sum_send.at[owner],
            dst_ref=sum_recv.at[me],
            send_sem=sum_sem.at[0],
            recv_sem=sum_sem.at[1],
            device_id={"dev": owner},
            device_id_type=MESH,
        ).start()
        return 0

    lax.fori_loop(1, N_DEV, small_sends, 0)
    send_qkv(partner)

    def qkv_sends(flip, _):
        for offsets in ROUNDS:
            send_qkv_round(offsets, flip)
        return 0

    lax.fori_loop(0, 2, qkv_sends, 0)
    gate_round(ROUNDS[2])
    gate_round(ROUNDS[3])
    gate_round(ROUNDS[4])

    sum_recv[me] = sum_send[me]
    qkv_land[own_rows] = qkv_send[me]

    row_of = lax.broadcasted_iota(jnp.int32, (8, STORED), 0)
    layer_of = lax.broadcasted_iota(jnp.int32, (8, STORED), 1)
    wanted = jnp.where(row_of == 0, layer_ref[0], layer_ref[1])
    layer_pick = jnp.where((layer_of == wanted) & (row_of < LAYERS), 1.0, 0.0).astype(jnp.float32)

    def picked(table, columns):
        dot = functools.partial(
            jnp.dot, precision=lax.Precision.HIGHEST, preferred_element_type=jnp.float32
        )
        return dot(dot(layer_pick, table.astype(jnp.float32)), columns)

    blocks = 2 * FF // BLK
    block_of = lax.broadcasted_iota(jnp.int32, (blocks, 128), 0)
    to = lax.broadcasted_iota(jnp.int32, (blocks, 128), 1)
    source = me * BLOCKS + jnp.where(to < BLOCKS, to, FF // BLK + to - BLOCKS)
    pick_g = jnp.where((block_of == source) & (to < 2 * BLOCKS), 1.0, 0.0).astype(jnp.float32)
    head_of = lax.broadcasted_iota(jnp.int32, (NHEAD, 128), 0)
    to = lax.broadcasted_iota(jnp.int32, (NHEAD, 128), 1)
    pick_q = jnp.zeros((NHEAD, 128), jnp.float32)
    for s in range(SLOTS):
        hit = (head_of == slot_ref[me * SLOTS + s]) & (to == 2 * BLOCKS + s)
        pick_q = jnp.where(hit, 1.0, pick_q)
    expected = (picked(table_g[...], pick_g) + picked(table_q[...], pick_q)) * stored_unit

    def take_apart(land, out, chip, column):
        start = pl.multiple_of(chip * 2 * ROWS, 8)
        rows = land[pl.ds(start, 2 * ROWS), :, column].reshape(2 * ROWS // 8, 8, LAYERS, BLK)
        rows = jnp.swapaxes(rows, 1, 2)
        for i in range(2 * ROWS // 8):
            for layer in range(LAYERS):
                out[layer, pl.ds(pl.multiple_of(start + 8 * i, 8), 8), column] = rows[i, layer]

    def chip_at(offset):
        x, y = me // 8, (me // 2) % 4
        return (x + offset[0] + 4) % 4 * 4 + (y + offset[1] + 4) % 4

    def settle(land, out, chip, first, width):
        def step(i, _):
            take_apart(land, out, chip, pl.ds(pl.multiple_of(first + i * BLK, BLK), BLK))
            return 0

        lax.fori_loop(0, width // BLK, step, 0)

    def settle_gate(offsets):
        for p in range(2):
            for offset in offsets:
                chip = chip_at(offset)
                for core in range(2):
                    source = chip * 2 + core
                    block = gate_land.at[pl.ds(source * ROWS, ROWS), :, pl.ds(p * WIDTH, WIDTH)]
                    pltpu.make_async_copy(block, block, gate_recv.at[source, p]).wait()
                settle(gate_land, gate_out, chip, p * WIDTH, WIDTH)

    def settle_qkv(offset):
        chip = chip_at(offset)
        for core in range(2):
            source = chip * 2 + core
            block = qkv_land.at[pl.ds(source * ROWS, ROWS)]
            pl.when(source != me)(pltpu.make_async_copy(block, block, qkv_recv.at[source]).wait)
        settle(qkv_land, qkv_out, chip, 0, QW)

    here = ((0, 0),)
    settle_gate(here)
    settle_gate(ROUNDS[0])
    settle_gate(ROUNDS[1])

    others = pl.ds(0, N_DEV - 1)
    pltpu.make_async_copy(sum_recv.at[others], sum_recv.at[others], sum_sem.at[1]).wait()
    part_send[...] = jnp.sum(sum_recv[...], axis=0)
    to_first = pltpu.make_async_remote_copy(
        src_ref=part_send,
        dst_ref=part_recv.at[grp],
        send_sem=part_sem.at[0],
        recv_sem=part_sem.at[1],
        device_id={"grp": 0},
        device_id_type=MESH,
    )

    @pl.when(grp > 0)
    def _():
        to_first.start()

    for offsets in (here,) + ROUNDS:
        for offset in offsets:
            settle_qkv(offset)
    parts = pl.ds(1, N_GRP - 1)
    from_others = part_recv.at[parts]

    def give(total):
        difference = total - expected[:LAYERS]
        gate_mismatch[...] = difference[:, : 2 * BLOCKS]
        qkv_mismatch[...] = difference[:, 2 * BLOCKS : 2 * BLOCKS + SLOTS]

    def total_to(k):
        return pltpu.make_async_remote_copy(
            src_ref=part_total,
            dst_ref=part_land,
            send_sem=part_sem.at[2],
            recv_sem=part_sem.at[3],
            device_id={"grp": k},
            device_id_type=MESH,
        )

    @pl.when(grp == 0)
    def _():
        part_recv[0] = part_send[...]
        pltpu.make_async_copy(from_others, from_others, part_sem.at[1]).wait()
        total = jnp.sum(part_recv[...], axis=0)
        part_total[...] = total
        give(total)
        for k in range(1, N_GRP):
            total_to(k).start()

    settle_gate(ROUNDS[2])
    settle_gate(ROUNDS[3])
    settle_gate(ROUNDS[4])

    @pl.when(grp > 0)
    def _():
        pltpu.make_async_copy(part_land, part_land, part_sem.at[3]).wait()
        give(part_land[...])
        to_first.wait_send()

    @pl.when(grp == 0)
    def _():
        pltpu.make_async_copy(from_others, from_others, part_sem.at[2]).wait()

    pltpu.make_async_copy(sum_recv.at[others], sum_recv.at[others], sum_sem.at[0]).wait()
    moved = pl.ds(0, (N_DEV - 1) * ROWS)
    pltpu.make_async_copy(qkv_land.at[moved], qkv_land.at[moved], qkv_sem).wait()
    pltpu.make_async_copy(gate_land.at[moved], gate_land.at[moved], gate_sem).wait()


def put_out(gate, qkv, qkv_mismatch, gate_mismatch, gate_out, qkv_out, qkv_m_out, gate_m_out, sem):
    height = N_DEV * ROWS // PIECES
    pairs = [
        (gate.at[layer, pl.ds(k * height, height)], gate_out.at[layer, pl.ds(k * height, height)])
        for layer in range(LAYERS)
        for k in range(PIECES)
    ]
    pairs += [(qkv, qkv_out), (qkv_mismatch, qkv_m_out), (gate_mismatch, gate_m_out)]
    copies = [pltpu.make_async_copy(a, b, sem.at[i]) for i, (a, b) in enumerate(pairs)]
    for copy in copies:
        copy.start()
    for copy in copies:
        copy.wait()


def body(qkv_weight, gate_up_weight, head_slot, layer_ids, stored_qkv, stored_gate_up):
    anywhere = pl.BlockSpec(memory_space=pl.ANY)
    in_vmem = pl.BlockSpec(memory_space=pltpu.VMEM)
    total_rows = N_DEV * ROWS
    landed = pl.pallas_call(
        kernel,
        out_shape=(
            pltpu.VMEM((LAYERS, total_rows, 2 * WIDTH), jnp.bfloat16),
            pltpu.VMEM((LAYERS, total_rows, QW), jnp.bfloat16),
            pltpu.VMEM((LAYERS, SLOTS), jnp.float32),
            pltpu.VMEM((LAYERS, 2 * BLOCKS), jnp.float32),
        ),
        in_specs=[anywhere] * 6,
        out_specs=(in_vmem,) * 4,
        scratch_shapes=[
            pltpu.VMEM((total_rows, LAYERS, 2 * WIDTH), jnp.bfloat16),
            pltpu.VMEM((total_rows, LAYERS, QW), jnp.bfloat16),
            pltpu.VMEM((NHEAD, ROWS, LAYERS, HEAD_DIM), jnp.bfloat16),
            pltpu.VMEM((N_DEV, ROWS, LAYERS, QW), jnp.bfloat16),
            pltpu.VMEM((2, 2, ROWS, LAYERS, WIDTH), jnp.bfloat16),
            pltpu.VMEM((N_DEV, LAYERS, 128), jnp.float32),
            pltpu.VMEM((N_DEV, LAYERS, 128), jnp.float32),
            pltpu.VMEM((LAYERS, 128), jnp.float32),
            pltpu.VMEM((N_GRP, LAYERS, 128), jnp.float32),
            pltpu.VMEM((LAYERS, 128), jnp.float32),
            pltpu.VMEM((LAYERS, 128), jnp.float32),
            pltpu.SMEM((NHEAD,), jnp.int32),
            pltpu.SMEM((LAYERS,), jnp.int32),
            pltpu.VMEM((STORED, NHEAD), jnp.int32),
            pltpu.VMEM((STORED, 2 * FF // BLK), jnp.int32),
            pltpu.SemaphoreType.DMA,
            pltpu.SemaphoreType.DMA((N_DEV, 2)),
            pltpu.SemaphoreType.DMA,
            pltpu.SemaphoreType.DMA((N_DEV,)),
            pltpu.SemaphoreType.DMA((2,)),
            pltpu.SemaphoreType.DMA((4,)),
            pltpu.SemaphoreType.DMA((2, 2)),
            pltpu.SemaphoreType.DMA((5,)),
        ],
        compiler_params=pltpu.CompilerParams(
            collective_id=0, has_side_effects=True, vmem_limit_bytes=50 << 20
        ),
        name="exchange",
    )(
        gate_up_weight.transpose(1, 0, 2),
        qkv_weight.transpose(1, 0, 2),
        head_slot,
        layer_ids,
        stored_qkv,
        stored_gate_up,
    )
    served_gate, served_qkv, qkv_mismatch, gate_mismatch = pl.pallas_call(
        put_out,
        out_shape=tuple(jax.ShapeDtypeStruct(a.shape, a.dtype) for a in landed),
        in_specs=[in_vmem] * 4,
        out_specs=(anywhere,) * 4,
        scratch_shapes=[pltpu.SemaphoreType.DMA((LAYERS * PIECES + 3,))],
        compiler_params=pltpu.CompilerParams(vmem_limit_bytes=1 << 20),
        name="put_out",
    )(*landed)
    return served_qkv, served_gate, qkv_mismatch, gate_mismatch


def solution(mesh):
    placed = (P(None, ("grp", "dev"), None), P(None, ("grp", "dev"), None), P(), P(), P(), P())
    return jax.shard_map(
        body,
        mesh=mesh,
        in_specs=placed,
        out_specs=(P(None, "grp", "dev"), P(None, "grp", "dev"), P(None, "dev"), P(None, "dev")),
        check_vma=False,
    )
```

```python
import functools

import jax
import jax.numpy as jnp
from jax import lax
from jax.experimental import pallas as pl
from jax.experimental.pallas import tpu as pltpu
from jax.sharding import PartitionSpec as P

HEAD_DIM = 128
FF = 36864
STORED = 46
BLK = 128
NHEAD = 64
LAYERS = 2
ROWS = 36
N_DEV = 32
N_GRP = 4
WIDTH = FF // N_DEV
BLOCKS = WIDTH // BLK
SLOTS = NHEAD // N_DEV
QW = SLOTS * HEAD_DIM
PIECES = 4
CHIP_ROWS = 2 * ROWS
VMEM_LIMIT = 38

stored_unit = 1.0 / 1024.0
MESH = pl.DeviceIdType.MESH

FAR_X = ((2, 1, 0, 1), (0, 1, 0, 1), (2, -1, 0, 1), (0, -1, 0, 1))
FAR_Y = ((1, 2, 1, 0), (-1, 0, 1, 0), (-1, 2, 1, 0), (1, 0, 1, 0))
DIAGONAL = ((1, 1, 0, 0), (-1, -1, 0, 0))
ANTIDIAGONAL = ((1, -1, 0, 0), (-1, 1, 0, 0))
OPPOSITE = ((2, 0, 0, 0), (0, 2, 0, 0), (2, 2, 0, 0))
ROUNDS = (FAR_X, OPPOSITE, FAR_Y, DIAGONAL, ANTIDIAGONAL)
LAST = DIAGONAL + ANTIDIAGONAL


FAR_FIRST = sorted(range(1, N_DEV), key=lambda k: -(min(k // 8, 4 - k // 8) + min(k // 2 % 4, 4 - k // 2 % 4)))


def owner_at(me, offset, flip):
    dx, dy, mirror_x, mirror_y = offset
    x, y, core = me // 8, (me // 2) % 4, me % 2
    sign = 1 - 2 * core
    x = (x + (dx * sign if mirror_x else dx) + 4) % 4
    y = (y + (dy * sign if mirror_y else dy) + 4) % 4
    return (x * 4 + y) * 2 + (core + flip) % 2


def kernel(
    gate, qkv, head_slot, layer_ids, stored_q, stored_g,
    gate_out, gate_land, qkv_out, qkv_mismatch, gate_mismatch,
    qkv_land,
    qkv_in, qkv_send, rows_in, sum_send, sum_recv, part_send, part_recv, part_total, part_land,
    slot_ref, layer_ref, table_q, table_g, gate_sem, gate_recv, qkv_sem, qkv_recv, sum_sem, part_sem, load_sem, table_sem,
):
    me = lax.axis_index("dev")
    grp = lax.axis_index("grp")

    barrier = pltpu.get_barrier_semaphore()

    for k in FAR_FIRST:
        pl.semaphore_signal(barrier, inc=1, device_id={"dev": (me + k) % N_DEV}, device_id_type=MESH)

    def greet_later(k, _):
        pl.semaphore_signal(barrier, inc=1, device_id={"grp": k}, device_id_type=MESH)
        return 0

    lax.fori_loop(grp + 1, N_GRP, greet_later, 0)
    pl.semaphore_wait(barrier, N_DEV - 1 + grp)

    own_rows = pl.ds(me * ROWS, ROWS)

    def send_gate(owner, p):
        pltpu.make_async_remote_copy(
            src_ref=gate.at[:, :, pl.ds(pl.multiple_of(p * FF + owner * WIDTH, BLK), WIDTH)],
            dst_ref=gate_land.at[own_rows, :, pl.ds(pl.multiple_of(p * WIDTH, BLK), WIDTH)],
            send_sem=gate_sem,
            recv_sem=gate_recv.at[me, p],
            device_id={"dev": owner},
            device_id_type=MESH,
        ).start()

    def send_qkv(owner):
        pltpu.make_async_remote_copy(
            src_ref=qkv_send.at[owner],
            dst_ref=qkv_land.at[own_rows],
            send_sem=qkv_sem,
            recv_sem=qkv_recv.at[me],
            device_id={"dev": owner},
            device_id_type=MESH,
        ).start()

    def gate_round(offsets):
        def step(i, _):
            for offset in offsets:
                send_gate(owner_at(me, offset, i % 2), i // 2)
            return 0

        lax.fori_loop(0, 4, step, 0)

    partner = owner_at(me, (0, 0, 0, 0), 1)
    for p in range(2):
        send_gate(partner, p)
    gate_round(ROUNDS[0])
    gate_round(ROUNDS[1])
    for p in range(2):
        pltpu.make_async_copy(
            gate.at[:, :, pl.ds(pl.multiple_of(p * FF + me * WIDTH, BLK), WIDTH)],
            gate_land.at[own_rows, :, pl.ds(p * WIDTH, WIDTH)],
            gate_recv.at[me, p],
        ).start()

    fetches = [
        pltpu.make_async_copy(source, target, table_sem.at[1 + i])
        for i, (source, target) in enumerate(
            ((head_slot, slot_ref), (layer_ids, layer_ref), (stored_q, table_q), (stored_g, table_g))
        )
    ]
    for fetch in fetches:
        fetch.start()

    def load_head(head, _):
        column = pl.ds(pl.multiple_of(head * HEAD_DIM, HEAD_DIM), HEAD_DIM)
        pltpu.make_async_copy(qkv.at[:, :, column], qkv_in.at[head], table_sem.at[0]).start()
        return 0

    lax.fori_loop(0, NHEAD, load_head, 0)
    for fetch in fetches:
        fetch.wait()
    pltpu.make_async_copy(qkv_in, qkv_in, table_sem.at[0]).wait()

    def place(slot, _):
        part = qkv_in[slot_ref[slot]]
        column = pl.ds(pl.multiple_of((slot % SLOTS) * HEAD_DIM, HEAD_DIM), HEAD_DIM)
        qkv_send[slot // SLOTS, :, :, column] = part
        return 0

    lax.fori_loop(0, NHEAD, place, 0)

    def load(owner, slot):
        return [
            pltpu.make_async_copy(
                gate.at[:, :, pl.ds(pl.multiple_of(p * FF + owner * WIDTH, BLK), WIDTH)],
                rows_in.at[slot, p],
                load_sem.at[slot, p],
            )
            for p in range(2)
        ]

    lane = lax.broadcasted_iota(jnp.int32, (LAYERS, 128), 1)

    def block_total(values, at, total):
        rows = jnp.sum(values.astype(jnp.float32), axis=0)
        return jnp.where(lane == at, jnp.sum(rows, axis=1, keepdims=True), total)

    for copy in load(0, 0):
        copy.start()

    def add_up(owner, _):
        slot = owner % 2

        @pl.when(owner + 1 < N_DEV)
        def _():
            for copy in load(owner + 1, 1 - slot):
                copy.start()

        for copy in load(owner, slot):
            copy.wait()
        total = jnp.zeros((LAYERS, 128), jnp.float32)
        for p in range(2):
            for b in range(BLOCKS):
                total = block_total(rows_in[slot, p, :, :, b * BLK : (b + 1) * BLK], p * BLOCKS + b, total)
        for s in range(SLOTS):
            total = block_total(
                qkv_send[owner, :, :, s * HEAD_DIM : (s + 1) * HEAD_DIM], 2 * BLOCKS + s, total
            )
        sum_send[owner] = total
        return 0

    lax.fori_loop(0, N_DEV, add_up, 0)

    def send_qkv_round(offsets, flip):
        for offset in offsets:
            send_qkv(owner_at(me, offset, flip))

    def small_sends(i, _):
        owner = (me + i) % N_DEV
        pltpu.make_async_remote_copy(
            src_ref=sum_send.at[owner],
            dst_ref=sum_recv.at[me],
            send_sem=sum_sem.at[0],
            recv_sem=sum_sem.at[1],
            device_id={"dev": owner},
            device_id_type=MESH,
        ).start()
        return 0

    send_qkv(partner)

    def qkv_sends(flip, _):
        for offsets in ROUNDS:
            send_qkv_round(offsets, flip)
        return 0

    lax.fori_loop(0, 2, qkv_sends, 0)
    lax.fori_loop(1, N_DEV, small_sends, 0)
    gate_round(ROUNDS[2])
    gate_round(ROUNDS[3])
    gate_round(ROUNDS[4])

    sum_recv[me] = sum_send[me]
    qkv_land[own_rows] = qkv_send[me]

    row_of = lax.broadcasted_iota(jnp.int32, (8, STORED), 0)
    layer_of = lax.broadcasted_iota(jnp.int32, (8, STORED), 1)
    wanted = jnp.where(row_of == 0, layer_ref[0], layer_ref[1])
    layer_pick = jnp.where((layer_of == wanted) & (row_of < LAYERS), 1.0, 0.0).astype(jnp.float32)

    def picked(table, columns):
        dot = functools.partial(
            jnp.dot, precision=lax.Precision.HIGHEST, preferred_element_type=jnp.float32
        )
        return dot(dot(layer_pick, table.astype(jnp.float32)), columns)

    blocks = 2 * FF // BLK
    block_of = lax.broadcasted_iota(jnp.int32, (blocks, 128), 0)
    to = lax.broadcasted_iota(jnp.int32, (blocks, 128), 1)
    source = me * BLOCKS + jnp.where(to < BLOCKS, to, FF // BLK + to - BLOCKS)
    pick_g = jnp.where((block_of == source) & (to < 2 * BLOCKS), 1.0, 0.0).astype(jnp.float32)
    head_of = lax.broadcasted_iota(jnp.int32, (NHEAD, 128), 0)
    to = lax.broadcasted_iota(jnp.int32, (NHEAD, 128), 1)
    pick_q = jnp.zeros((NHEAD, 128), jnp.float32)
    for s in range(SLOTS):
        hit = (head_of == slot_ref[me * SLOTS + s]) & (to == 2 * BLOCKS + s)
        pick_q = jnp.where(hit, 1.0, pick_q)
    expected = (picked(table_g[...], pick_g) + picked(table_q[...], pick_q)) * stored_unit

    def settle(land, out, chip, first, width):
        def step(i, _):
            column = pl.ds(pl.multiple_of(first + i * BLK, BLK), BLK)
            rows = take_apart(land, chip, column)
            for k in range(CHIP_ROWS // 8):
                for layer in range(LAYERS):
                    out[layer, pl.ds(pl.multiple_of(chip * CHIP_ROWS + 8 * k, 8), 8), column] = rows[k, layer]
            return 0

        lax.fori_loop(0, width // BLK, step, 0)

    def settle_gate(offsets, last=False):
        for p in range(2):
            for offset in offsets:
                chip = chip_at(me, offset)
                for core in range(2):
                    source = chip * 2 + core
                    block = gate_land.at[pl.ds(source * ROWS, ROWS), :, pl.ds(p * WIDTH, WIDTH)]
                    pltpu.make_async_copy(block, block, gate_recv.at[source, p]).wait()
                if not (last and p):
                    settle(gate_land, gate_out, chip, p * WIDTH, WIDTH)

    def settle_qkv(offset):
        chip = chip_at(me, offset)
        for core in range(2):
            source = chip * 2 + core
            block = qkv_land.at[pl.ds(source * ROWS, ROWS)]
            pl.when(source != me)(pltpu.make_async_copy(block, block, qkv_recv.at[source]).wait)
        settle(qkv_land, qkv_out, chip, 0, QW)

    here = ((0, 0),)
    settle_gate(here)
    settle_gate(ROUNDS[0])
    settle_gate(ROUNDS[1])

    others = pl.ds(0, N_DEV - 1)
    pltpu.make_async_copy(sum_recv.at[others], sum_recv.at[others], sum_sem.at[1]).wait()
    part_send[...] = jnp.sum(sum_recv[...], axis=0)
    to_first = pltpu.make_async_remote_copy(
        src_ref=part_send,
        dst_ref=part_recv.at[grp],
        send_sem=part_sem.at[0],
        recv_sem=part_sem.at[1],
        device_id={"grp": 0},
        device_id_type=MESH,
    )

    for offset in here + ROUNDS[0]:
        settle_qkv(offset)

    @pl.when(grp > 0)
    def _():
        to_first.start()

    for offsets in ROUNDS[1:]:
        for offset in offsets:
            settle_qkv(offset)
    parts = pl.ds(1, N_GRP - 1)
    from_others = part_recv.at[parts]

    def give(total):
        difference = total - expected[:LAYERS]
        gate_mismatch[...] = difference[:, : 2 * BLOCKS]
        qkv_mismatch[...] = difference[:, 2 * BLOCKS : 2 * BLOCKS + SLOTS]

    def total_to(k):
        return pltpu.make_async_remote_copy(
            src_ref=part_total,
            dst_ref=part_land,
            send_sem=part_sem.at[2],
            recv_sem=part_sem.at[3],
            device_id={"grp": k},
            device_id_type=MESH,
        )

    @pl.when(grp == 0)
    def _():
        part_recv[0] = part_send[...]
        pltpu.make_async_copy(from_others, from_others, part_sem.at[1]).wait()
        total = jnp.sum(part_recv[...], axis=0)
        part_total[...] = total
        give(total)
    settle_gate(ROUNDS[2])

    @pl.when(grp == 0)
    def _():
        for k in range(1, N_GRP):
            total_to(k).start()

    settle_gate(LAST, last=True)

    @pl.when(grp > 0)
    def _():
        pltpu.make_async_copy(part_land, part_land, part_sem.at[3]).wait()
        give(part_land[...])
        to_first.wait_send()

    @pl.when(grp == 0)
    def _():
        pltpu.make_async_copy(from_others, from_others, part_sem.at[2]).wait()

    pltpu.make_async_copy(sum_recv.at[others], sum_recv.at[others], sum_sem.at[0]).wait()
    moved = pl.ds(0, (N_DEV - 1) * ROWS)
    pltpu.make_async_copy(qkv_land.at[moved], qkv_land.at[moved], qkv_sem).wait()
    pltpu.make_async_copy(gate_land.at[moved], gate_land.at[moved], gate_sem).wait()


def take_apart(land, chip, column):
    rows = land[pl.ds(pl.multiple_of(chip * CHIP_ROWS, 8), CHIP_ROWS), :, column]
    return jnp.swapaxes(rows.reshape(CHIP_ROWS // 8, 8, LAYERS, BLK), 1, 2)


def chip_at(me, offset):
    x, y = me // 8, (me // 2) % 4
    return (x + offset[0] + 4) % 4 * 4 + (y + offset[1] + 4) % 4


def put_out(gate, land, qkv, qkv_mismatch, gate_mismatch, gate_out, qkv_out, qkv_m_out, gate_m_out, rest, sem):
    me = lax.axis_index("dev")
    gate_columns, up_columns = pl.ds(0, WIDTH), pl.ds(WIDTH, WIDTH)
    last = [chip_at(me, offset) for offset in LAST]
    height = N_DEV * ROWS // PIECES
    copies = [
        pltpu.make_async_copy(
            gate.at[layer, pl.ds(k * height, height), gate_columns],
            gate_out.at[layer, pl.ds(k * height, height), gate_columns],
            sem.at[layer * PIECES + k],
        )
        for layer in range(LAYERS)
        for k in range(PIECES)
    ]
    small = ((qkv, qkv_out), (qkv_mismatch, qkv_m_out), (gate_mismatch, gate_m_out))
    copies += [pltpu.make_async_copy(a, b, sem.at[LAYERS * PIECES + i]) for i, (a, b) in enumerate(small)]
    first_up = len(copies)

    def up(chip, source):
        rows = pl.ds(pl.multiple_of(chip * CHIP_ROWS, 8), CHIP_ROWS)
        target = gate_out.at[:, rows, up_columns]
        return pltpu.make_async_copy(
            gate.at[:, rows, up_columns] if source is None else source, target, sem.at[first_up + chip]
        )

    for copy in copies:
        copy.start()

    def start_up(chip, _):
        left = (chip != last[0]) & (chip != last[1]) & (chip != last[2]) & (chip != last[3])

        @pl.when(left)
        def _():
            up(chip, None).start()

        return 0

    lax.fori_loop(0, N_DEV // 2, start_up, 0)
    for at, chip in enumerate(last):

        def step(i, _):
            rows = take_apart(land, chip, pl.ds(pl.multiple_of(WIDTH + i * BLK, BLK), BLK))
            for k in range(CHIP_ROWS // 8):
                for layer in range(LAYERS):
                    rest[at, layer, pl.ds(8 * k, 8), pl.ds(pl.multiple_of(i * BLK, BLK), BLK)] = rows[k, layer]
            return 0

        lax.fori_loop(0, BLOCKS, step, 0)
    for at, chip in enumerate(last):
        up(chip, rest.at[at]).start()
    for copy in copies:
        copy.wait()

    def end_up(chip, _):
        up(chip, None).wait()
        return 0

    lax.fori_loop(0, N_DEV // 2, end_up, 0)


def body(qkv_weight, gate_up_weight, head_slot, layer_ids, stored_qkv, stored_gate_up):
    anywhere = pl.BlockSpec(memory_space=pl.ANY)
    in_vmem = pl.BlockSpec(memory_space=pltpu.VMEM)
    total_rows = N_DEV * ROWS
    landed = pl.pallas_call(
        kernel,
        out_shape=(
            pltpu.VMEM((LAYERS, total_rows, 2 * WIDTH), jnp.bfloat16),
            pltpu.VMEM((total_rows, LAYERS, 2 * WIDTH), jnp.bfloat16),
            pltpu.VMEM((LAYERS, total_rows, QW), jnp.bfloat16),
            pltpu.VMEM((LAYERS, SLOTS), jnp.float32),
            pltpu.VMEM((LAYERS, 2 * BLOCKS), jnp.float32),
        ),
        in_specs=[anywhere] * 6,
        out_specs=(in_vmem,) * 5,
        scratch_shapes=[
            pltpu.VMEM((total_rows, LAYERS, QW), jnp.bfloat16),
            pltpu.VMEM((NHEAD, ROWS, LAYERS, HEAD_DIM), jnp.bfloat16),
            pltpu.VMEM((N_DEV, ROWS, LAYERS, QW), jnp.bfloat16),
            pltpu.VMEM((2, 2, ROWS, LAYERS, WIDTH), jnp.bfloat16),
            pltpu.VMEM((N_DEV, LAYERS, 128), jnp.float32),
            pltpu.VMEM((N_DEV, LAYERS, 128), jnp.float32),
            pltpu.VMEM((LAYERS, 128), jnp.float32),
            pltpu.VMEM((N_GRP, LAYERS, 128), jnp.float32),
            pltpu.VMEM((LAYERS, 128), jnp.float32),
            pltpu.VMEM((LAYERS, 128), jnp.float32),
            pltpu.SMEM((NHEAD,), jnp.int32),
            pltpu.SMEM((LAYERS,), jnp.int32),
            pltpu.VMEM((STORED, NHEAD), jnp.int32),
            pltpu.VMEM((STORED, 2 * FF // BLK), jnp.int32),
            pltpu.SemaphoreType.DMA,
            pltpu.SemaphoreType.DMA((N_DEV, 2)),
            pltpu.SemaphoreType.DMA,
            pltpu.SemaphoreType.DMA((N_DEV,)),
            pltpu.SemaphoreType.DMA((2,)),
            pltpu.SemaphoreType.DMA((4,)),
            pltpu.SemaphoreType.DMA((2, 2)),
            pltpu.SemaphoreType.DMA((5,)),
        ],
        compiler_params=pltpu.CompilerParams(
            collective_id=0, has_side_effects=True, vmem_limit_bytes=VMEM_LIMIT << 20
        ),
        name="exchange",
    )(
        gate_up_weight.transpose(1, 0, 2),
        qkv_weight.transpose(1, 0, 2),
        head_slot,
        layer_ids,
        stored_qkv,
        stored_gate_up,
    )
    served_gate, served_qkv, qkv_mismatch, gate_mismatch = pl.pallas_call(
        put_out,
        out_shape=tuple(jax.ShapeDtypeStruct(a.shape, a.dtype) for a in landed[:1] + landed[2:]),
        in_specs=[in_vmem] * 5,
        out_specs=(anywhere,) * 4,
        scratch_shapes=[
            pltpu.VMEM((len(LAST), LAYERS, CHIP_ROWS, WIDTH), jnp.bfloat16),
            pltpu.SemaphoreType.DMA((LAYERS * PIECES + 3 + N_DEV // 2,)),
        ],
        compiler_params=pltpu.CompilerParams(vmem_limit_bytes=8 << 20),
        name="put_out",
    )(*landed)
    return served_qkv, served_gate, qkv_mismatch, gate_mismatch


def solution(mesh):
    placed = (P(None, ("grp", "dev"), None), P(None, ("grp", "dev"), None), P(), P(), P(), P())
    return jax.shard_map(
        body,
        mesh=mesh,
        in_specs=placed,
        out_specs=(P(None, "grp", "dev"), P(None, "grp", "dev"), P(None, "dev"), P(None, "dev")),
        check_vma=False,
    )
```

```python
import functools

import jax
import jax.numpy as jnp
from jax import lax
from jax.experimental import pallas as pl
from jax.experimental.pallas import tpu as pltpu
from jax.sharding import PartitionSpec as P

HEAD_DIM = 128
FF = 36864
STORED = 46
BLK = 128
NHEAD = 64
LAYERS = 2
ROWS = 36
N_DEV = 32
N_GRP = 4
WIDTH = FF // N_DEV
BLOCKS = WIDTH // BLK
SLOTS = NHEAD // N_DEV
QW = SLOTS * HEAD_DIM
PIECES = 4
CHIP_ROWS = 2 * ROWS
VMEM_LIMIT = 38

stored_unit = 1.0 / 1024.0
MESH = pl.DeviceIdType.MESH

FAR_X = ((2, 1, 0, 1), (0, 1, 0, 1), (2, -1, 0, 1), (0, -1, 0, 1))
FAR_Y = ((1, 2, 1, 0), (-1, 0, 1, 0), (-1, 2, 1, 0), (1, 0, 1, 0))
DIAGONAL = ((1, 1, 0, 0), (-1, -1, 0, 0))
ANTIDIAGONAL = ((1, -1, 0, 0), (-1, 1, 0, 0))
OPPOSITE = ((2, 0, 0, 0), (0, 2, 0, 0), (2, 2, 0, 0))
ROUNDS = (FAR_X, OPPOSITE, FAR_Y, DIAGONAL, ANTIDIAGONAL)
LAST = DIAGONAL + ANTIDIAGONAL


FAR_FIRST = sorted(range(1, N_DEV), key=lambda k: -(min(k // 8, 4 - k // 8) + min(k // 2 % 4, 4 - k // 2 % 4)))


def owner_at(me, offset, flip):
    dx, dy, mirror_x, mirror_y = offset
    x, y, core = me // 8, (me // 2) % 4, me % 2
    sign = 1 - 2 * core
    x = (x + (dx * sign if mirror_x else dx) + 4) % 4
    y = (y + (dy * sign if mirror_y else dy) + 4) % 4
    return (x * 4 + y) * 2 + (core + flip) % 2


def kernel(
    gate, qkv, head_slot, layer_ids, stored_q, stored_g,
    gate_out, gate_land, qkv_out, qkv_mismatch, gate_mismatch,
    qkv_land,
    qkv_in, qkv_send, rows_in, sum_send, sum_recv, part_send, part_recv, part_total, part_land,
    slot_ref, layer_ref, table_q, table_g, gate_sem, gate_recv, qkv_sem, qkv_recv, sum_sem, part_sem, load_sem, table_sem,
):
    me = lax.axis_index("dev")
    grp = lax.axis_index("grp")

    barrier = pltpu.get_barrier_semaphore()

    for k in FAR_FIRST:
        pl.semaphore_signal(barrier, inc=1, device_id={"dev": (me + k) % N_DEV}, device_id_type=MESH)

    def greet_later(k, _):
        pl.semaphore_signal(barrier, inc=1, device_id={"grp": k}, device_id_type=MESH)
        return 0

    lax.fori_loop(grp + 1, N_GRP, greet_later, 0)
    pl.semaphore_wait(barrier, N_DEV - 1 + grp)

    own_rows = pl.ds(me * ROWS, ROWS)

    def send_gate(owner, p):
        pltpu.make_async_remote_copy(
            src_ref=gate.at[:, :, pl.ds(pl.multiple_of(p * FF + owner * WIDTH, BLK), WIDTH)],
            dst_ref=gate_land.at[own_rows, :, pl.ds(pl.multiple_of(p * WIDTH, BLK), WIDTH)],
            send_sem=gate_sem,
            recv_sem=gate_recv.at[me, p],
            device_id={"dev": owner},
            device_id_type=MESH,
        ).start()

    def send_qkv(owner):
        pltpu.make_async_remote_copy(
            src_ref=qkv_send.at[owner],
            dst_ref=qkv_land.at[own_rows],
            send_sem=qkv_sem,
            recv_sem=qkv_recv.at[me],
            device_id={"dev": owner},
            device_id_type=MESH,
        ).start()

    def gate_round(offsets):
        def step(i, _):
            for offset in offsets:
                send_gate(owner_at(me, offset, i % 2), i // 2)
            return 0

        lax.fori_loop(0, 4, step, 0)

    partner = owner_at(me, (0, 0, 0, 0), 1)
    for p in range(2):
        send_gate(partner, p)
    gate_round(ROUNDS[0])
    gate_round(ROUNDS[1])
    gate_round(ROUNDS[2])
    for p in range(2):
        pltpu.make_async_copy(
            gate.at[:, :, pl.ds(pl.multiple_of(p * FF + me * WIDTH, BLK), WIDTH)],
            gate_land.at[own_rows, :, pl.ds(p * WIDTH, WIDTH)],
            gate_recv.at[me, p],
        ).start()

    fetches = [
        pltpu.make_async_copy(source, target, table_sem.at[1 + i])
        for i, (source, target) in enumerate(
            ((head_slot, slot_ref), (layer_ids, layer_ref), (stored_q, table_q), (stored_g, table_g))
        )
    ]
    for fetch in fetches:
        fetch.start()

    def load_head(head, _):
        column = pl.ds(pl.multiple_of(head * HEAD_DIM, HEAD_DIM), HEAD_DIM)
        pltpu.make_async_copy(qkv.at[:, :, column], qkv_in.at[head], table_sem.at[0]).start()
        return 0

    lax.fori_loop(0, NHEAD, load_head, 0)
    for fetch in fetches:
        fetch.wait()
    pltpu.make_async_copy(qkv_in, qkv_in, table_sem.at[0]).wait()

    def place(slot, _):
        part = qkv_in[slot_ref[slot]]
        column = pl.ds(pl.multiple_of((slot % SLOTS) * HEAD_DIM, HEAD_DIM), HEAD_DIM)
        qkv_send[slot // SLOTS, :, :, column] = part
        return 0

    lax.fori_loop(0, NHEAD, place, 0)

    def load(owner, slot):
        return [
            pltpu.make_async_copy(
                gate.at[:, :, pl.ds(pl.multiple_of(p * FF + owner * WIDTH, BLK), WIDTH)],
                rows_in.at[slot, p],
                load_sem.at[slot, p],
            )
            for p in range(2)
        ]

    lane = lax.broadcasted_iota(jnp.int32, (LAYERS, 128), 1)

    def block_total(values, at, total):
        rows = jnp.sum(values.astype(jnp.float32), axis=0)
        return jnp.where(lane == at, jnp.sum(rows, axis=1, keepdims=True), total)

    for copy in load(0, 0):
        copy.start()

    def add_up(owner, _):
        slot = owner % 2

        @pl.when(owner + 1 < N_DEV)
        def _():
            for copy in load(owner + 1, 1 - slot):
                copy.start()

        for copy in load(owner, slot):
            copy.wait()
        total = jnp.zeros((LAYERS, 128), jnp.float32)
        for p in range(2):
            for b in range(BLOCKS):
                total = block_total(rows_in[slot, p, :, :, b * BLK : (b + 1) * BLK], p * BLOCKS + b, total)
        for s in range(SLOTS):
            total = block_total(
                qkv_send[owner, :, :, s * HEAD_DIM : (s + 1) * HEAD_DIM], 2 * BLOCKS + s, total
            )
        sum_send[owner] = total
        return 0

    lax.fori_loop(0, N_DEV, add_up, 0)

    def send_qkv_round(offsets, flip):
        for offset in offsets:
            send_qkv(owner_at(me, offset, flip))

    def small_sends(i, _):
        owner = (me + i) % N_DEV
        pltpu.make_async_remote_copy(
            src_ref=sum_send.at[owner],
            dst_ref=sum_recv.at[me],
            send_sem=sum_sem.at[0],
            recv_sem=sum_sem.at[1],
            device_id={"dev": owner},
            device_id_type=MESH,
        ).start()
        return 0

    send_qkv(partner)

    def qkv_sends(flip, _):
        for offsets in ROUNDS:
            send_qkv_round(offsets, flip)
        return 0

    lax.fori_loop(0, 2, qkv_sends, 0)
    lax.fori_loop(1, N_DEV, small_sends, 0)
    gate_round(ROUNDS[3])
    gate_round(ROUNDS[4])

    sum_recv[me] = sum_send[me]
    qkv_land[own_rows] = qkv_send[me]

    row_of = lax.broadcasted_iota(jnp.int32, (8, STORED), 0)
    layer_of = lax.broadcasted_iota(jnp.int32, (8, STORED), 1)
    wanted = jnp.where(row_of == 0, layer_ref[0], layer_ref[1])
    layer_pick = jnp.where((layer_of == wanted) & (row_of < LAYERS), 1.0, 0.0).astype(jnp.float32)

    def picked(table, columns):
        dot = functools.partial(
            jnp.dot, precision=lax.Precision.HIGHEST, preferred_element_type=jnp.float32
        )
        return dot(dot(layer_pick, table.astype(jnp.float32)), columns)

    blocks = 2 * FF // BLK
    block_of = lax.broadcasted_iota(jnp.int32, (blocks, 128), 0)
    to = lax.broadcasted_iota(jnp.int32, (blocks, 128), 1)
    source = me * BLOCKS + jnp.where(to < BLOCKS, to, FF // BLK + to - BLOCKS)
    pick_g = jnp.where((block_of == source) & (to < 2 * BLOCKS), 1.0, 0.0).astype(jnp.float32)
    head_of = lax.broadcasted_iota(jnp.int32, (NHEAD, 128), 0)
    to = lax.broadcasted_iota(jnp.int32, (NHEAD, 128), 1)
    pick_q = jnp.zeros((NHEAD, 128), jnp.float32)
    for s in range(SLOTS):
        hit = (head_of == slot_ref[me * SLOTS + s]) & (to == 2 * BLOCKS + s)
        pick_q = jnp.where(hit, 1.0, pick_q)
    expected = (picked(table_g[...], pick_g) + picked(table_q[...], pick_q)) * stored_unit

    def settle(land, out, chip, first, width):
        def step(i, _):
            column = pl.ds(pl.multiple_of(first + i * BLK, BLK), BLK)
            rows = take_apart(land, chip, column)
            for k in range(CHIP_ROWS // 8):
                for layer in range(LAYERS):
                    out[layer, pl.ds(pl.multiple_of(chip * CHIP_ROWS + 8 * k, 8), 8), column] = rows[k, layer]
            return 0

        lax.fori_loop(0, width // BLK, step, 0)

    def settle_gate(offsets, last=False):
        for p in range(2):
            for offset in offsets:
                chip = chip_at(me, offset)
                for core in range(2):
                    source = chip * 2 + core
                    block = gate_land.at[pl.ds(source * ROWS, ROWS), :, pl.ds(p * WIDTH, WIDTH)]
                    pltpu.make_async_copy(block, block, gate_recv.at[source, p]).wait()
                if not (last and p):
                    settle(gate_land, gate_out, chip, p * WIDTH, WIDTH)

    def settle_qkv(offset):
        chip = chip_at(me, offset)
        for core in range(2):
            source = chip * 2 + core
            block = qkv_land.at[pl.ds(source * ROWS, ROWS)]
            pl.when(source != me)(pltpu.make_async_copy(block, block, qkv_recv.at[source]).wait)
        settle(qkv_land, qkv_out, chip, 0, QW)

    here = ((0, 0),)
    settle_gate(here)
    settle_gate(ROUNDS[0])
    settle_gate(ROUNDS[1])

    others = pl.ds(0, N_DEV - 1)
    pltpu.make_async_copy(sum_recv.at[others], sum_recv.at[others], sum_sem.at[1]).wait()
    part_send[...] = jnp.sum(sum_recv[...], axis=0)
    to_first = pltpu.make_async_remote_copy(
        src_ref=part_send,
        dst_ref=part_recv.at[grp],
        send_sem=part_sem.at[0],
        recv_sem=part_sem.at[1],
        device_id={"grp": 0},
        device_id_type=MESH,
    )

    for offset in here + ROUNDS[0]:
        settle_qkv(offset)

    @pl.when(grp > 0)
    def _():
        to_first.start()

    for offsets in ROUNDS[1:]:
        for offset in offsets:
            settle_qkv(offset)
    parts = pl.ds(1, N_GRP - 1)
    from_others = part_recv.at[parts]

    def give(total):
        difference = total - expected[:LAYERS]
        gate_mismatch[...] = difference[:, : 2 * BLOCKS]
        qkv_mismatch[...] = difference[:, 2 * BLOCKS : 2 * BLOCKS + SLOTS]

    def total_to(k):
        return pltpu.make_async_remote_copy(
            src_ref=part_total,
            dst_ref=part_land,
            send_sem=part_sem.at[2],
            recv_sem=part_sem.at[3],
            device_id={"grp": k},
            device_id_type=MESH,
        )

    @pl.when(grp == 0)
    def _():
        part_recv[0] = part_send[...]
        pltpu.make_async_copy(from_others, from_others, part_sem.at[1]).wait()
        total = jnp.sum(part_recv[...], axis=0)
        part_total[...] = total
        give(total)
    settle_gate(ROUNDS[2])

    @pl.when(grp == 0)
    def _():
        for k in range(1, N_GRP):
            total_to(k).start()

    settle_gate(LAST, last=True)

    @pl.when(grp > 0)
    def _():
        pltpu.make_async_copy(part_land, part_land, part_sem.at[3]).wait()
        give(part_land[...])
        to_first.wait_send()

    @pl.when(grp == 0)
    def _():
        pltpu.make_async_copy(from_others, from_others, part_sem.at[2]).wait()

    pltpu.make_async_copy(sum_recv.at[others], sum_recv.at[others], sum_sem.at[0]).wait()
    moved = pl.ds(0, (N_DEV - 1) * ROWS)
    pltpu.make_async_copy(qkv_land.at[moved], qkv_land.at[moved], qkv_sem).wait()
    pltpu.make_async_copy(gate_land.at[moved], gate_land.at[moved], gate_sem).wait()


def take_apart(land, chip, column):
    rows = land[pl.ds(pl.multiple_of(chip * CHIP_ROWS, 8), CHIP_ROWS), :, column]
    return jnp.swapaxes(rows.reshape(CHIP_ROWS // 8, 8, LAYERS, BLK), 1, 2)


def chip_at(me, offset):
    x, y = me // 8, (me // 2) % 4
    return (x + offset[0] + 4) % 4 * 4 + (y + offset[1] + 4) % 4


def put_out(gate, land, qkv, qkv_mismatch, gate_mismatch, gate_out, qkv_out, qkv_m_out, gate_m_out, rest, sem):
    me = lax.axis_index("dev")
    gate_columns, up_columns = pl.ds(0, WIDTH), pl.ds(WIDTH, WIDTH)
    last = [chip_at(me, offset) for offset in LAST]
    height = N_DEV * ROWS // PIECES
    copies = [
        pltpu.make_async_copy(
            gate.at[layer, pl.ds(k * height, height), gate_columns],
            gate_out.at[layer, pl.ds(k * height, height), gate_columns],
            sem.at[layer * PIECES + k],
        )
        for layer in range(LAYERS)
        for k in range(PIECES)
    ]
    small = ((qkv, qkv_out), (qkv_mismatch, qkv_m_out), (gate_mismatch, gate_m_out))
    copies += [pltpu.make_async_copy(a, b, sem.at[LAYERS * PIECES + i]) for i, (a, b) in enumerate(small)]
    first_up = len(copies)

    def up(chip, source):
        rows = pl.ds(pl.multiple_of(chip * CHIP_ROWS, 8), CHIP_ROWS)
        target = gate_out.at[:, rows, up_columns]
        return pltpu.make_async_copy(
            gate.at[:, rows, up_columns] if source is None else source, target, sem.at[first_up + chip]
        )

    for copy in copies:
        copy.start()

    def start_up(chip, _):
        left = (chip != last[0]) & (chip != last[1]) & (chip != last[2]) & (chip != last[3])

        @pl.when(left)
        def _():
            up(chip, None).start()

        return 0

    lax.fori_loop(0, N_DEV // 2, start_up, 0)
    for at, chip in enumerate(last):

        def step(i, _):
            rows = take_apart(land, chip, pl.ds(pl.multiple_of(WIDTH + i * BLK, BLK), BLK))
            for k in range(CHIP_ROWS // 8):
                for layer in range(LAYERS):
                    rest[at, layer, pl.ds(8 * k, 8), pl.ds(pl.multiple_of(i * BLK, BLK), BLK)] = rows[k, layer]
            return 0

        lax.fori_loop(0, BLOCKS, step, 0)
    for at, chip in enumerate(last):
        up(chip, rest.at[at]).start()
    for copy in copies:
        copy.wait()

    def end_up(chip, _):
        up(chip, None).wait()
        return 0

    lax.fori_loop(0, N_DEV // 2, end_up, 0)


def body(qkv_weight, gate_up_weight, head_slot, layer_ids, stored_qkv, stored_gate_up):
    anywhere = pl.BlockSpec(memory_space=pl.ANY)
    in_vmem = pl.BlockSpec(memory_space=pltpu.VMEM)
    total_rows = N_DEV * ROWS
    landed = pl.pallas_call(
        kernel,
        out_shape=(
            pltpu.VMEM((LAYERS, total_rows, 2 * WIDTH), jnp.bfloat16),
            pltpu.VMEM((total_rows, LAYERS, 2 * WIDTH), jnp.bfloat16),
            pltpu.VMEM((LAYERS, total_rows, QW), jnp.bfloat16),
            pltpu.VMEM((LAYERS, SLOTS), jnp.float32),
            pltpu.VMEM((LAYERS, 2 * BLOCKS), jnp.float32),
        ),
        in_specs=[anywhere] * 6,
        out_specs=(in_vmem,) * 5,
        scratch_shapes=[
            pltpu.VMEM((total_rows, LAYERS, QW), jnp.bfloat16),
            pltpu.VMEM((NHEAD, ROWS, LAYERS, HEAD_DIM), jnp.bfloat16),
            pltpu.VMEM((N_DEV, ROWS, LAYERS, QW), jnp.bfloat16),
            pltpu.VMEM((2, 2, ROWS, LAYERS, WIDTH), jnp.bfloat16),
            pltpu.VMEM((N_DEV, LAYERS, 128), jnp.float32),
            pltpu.VMEM((N_DEV, LAYERS, 128), jnp.float32),
            pltpu.VMEM((LAYERS, 128), jnp.float32),
            pltpu.VMEM((N_GRP, LAYERS, 128), jnp.float32),
            pltpu.VMEM((LAYERS, 128), jnp.float32),
            pltpu.VMEM((LAYERS, 128), jnp.float32),
            pltpu.SMEM((NHEAD,), jnp.int32),
            pltpu.SMEM((LAYERS,), jnp.int32),
            pltpu.VMEM((STORED, NHEAD), jnp.int32),
            pltpu.VMEM((STORED, 2 * FF // BLK), jnp.int32),
            pltpu.SemaphoreType.DMA,
            pltpu.SemaphoreType.DMA((N_DEV, 2)),
            pltpu.SemaphoreType.DMA,
            pltpu.SemaphoreType.DMA((N_DEV,)),
            pltpu.SemaphoreType.DMA((2,)),
            pltpu.SemaphoreType.DMA((4,)),
            pltpu.SemaphoreType.DMA((2, 2)),
            pltpu.SemaphoreType.DMA((5,)),
        ],
        compiler_params=pltpu.CompilerParams(
            collective_id=0, has_side_effects=True, vmem_limit_bytes=VMEM_LIMIT << 20
        ),
        name="exchange",
    )(
        gate_up_weight.transpose(1, 0, 2),
        qkv_weight.transpose(1, 0, 2),
        head_slot,
        layer_ids,
        stored_qkv,
        stored_gate_up,
    )
    served_gate, served_qkv, qkv_mismatch, gate_mismatch = pl.pallas_call(
        put_out,
        out_shape=tuple(jax.ShapeDtypeStruct(a.shape, a.dtype) for a in landed[:1] + landed[2:]),
        in_specs=[in_vmem] * 5,
        out_specs=(anywhere,) * 4,
        scratch_shapes=[
            pltpu.VMEM((len(LAST), LAYERS, CHIP_ROWS, WIDTH), jnp.bfloat16),
            pltpu.SemaphoreType.DMA((LAYERS * PIECES + 3 + N_DEV // 2,)),
        ],
        compiler_params=pltpu.CompilerParams(vmem_limit_bytes=8 << 20),
        name="put_out",
    )(*landed)
    return served_qkv, served_gate, qkv_mismatch, gate_mismatch


def solution(mesh):
    placed = (P(None, ("grp", "dev"), None), P(None, ("grp", "dev"), None), P(), P(), P(), P())
    return jax.shard_map(
        body,
        mesh=mesh,
        in_specs=placed,
        out_specs=(P(None, "grp", "dev"), P(None, "grp", "dev"), P(None, "dev"), P(None, "dev")),
        check_vma=False,
    )
```
